128 devices in a mesh: row: 8 (over x, core), col: 16 (over y, z).
Axes of the slice: x: 4, y: 4, z: 4, core: 2. Of those that a mesh axis runs over, the one named last changes fastest.
Arguments:
- velocity: float32 [3, 2, 128, 512, 256], P(None, None, 'row', 'col'), may hold values from -6 to 6
- register: float32 [3, 2, 128, 512, 256], P(None, None, 'row', 'col'), may hold values from -6 to 6
- offsets: int32 [256], replicated, may hold values from -2 to 2, as said below
- remesh_flag: int32 [256], replicated, may hold values from 0 to 1, as said below
- keep_blocks: int32 [16], replicated, may hold values 0 or 1
Outputs:
- velocity_next: float32 [3, 2, 128, 512, 256], P(None, None, 'row', 'col')
The draws below stay inside these ranges and needn't reach their ends.
Inputs may be any that keep to these rules, and one draw needn't show every extreme that they name: offsets[j] is 0 or has the sign of ky = j - 128. On each side of ky = 0 the planes of magnitude 1 form one run of consecutive ky, and the planes of magnitude 2 the run that follows it directly, farther from ky = 0. Each of -2, -1, 1 and 2 is carried by half of 32 to 32 planes. Each nonzero value of offsets[j] remesh_flag[j] is taken by at most 32 planes, and in every draw one of them by exactly 32 planes.
All inputs are finite; a program needn't handle non-finite values.
Results may differ from the reference program's by a relative error of at most 0.0055.
Values may be sent and summed in bfloat16 or wider, within the bound.
No kernel may reach another device: no remote copies, remote signals or barrier semaphores. Data moves between devices by JAX's collectives and lax.ppermute only.
A program may use at most 192 MiB of HBM per device.

```python
import math
import jax
import jax.numpy as jnp
from jax import lax

NX = 512
NY = 256
NZ = 256
NZH = 128
MX = 768
MY = 384
MZ = 384
KXB = 32
NBLK = 16
SHIFT_CAP = 32


def remesh_plan(key):
    folded = jax.random.fold_in(key, 4721)
    key_counts, key_pick, key_upper, key_lower, key_flag = jax.random.split(folded, 5)
    counts = jax.random.randint(key_counts, (4,), SHIFT_CAP // 2, SHIFT_CAP + 1).astype(jnp.int32)
    chosen = jax.random.randint(key_pick, (), 0, 4).astype(jnp.int32)
    slot_order = jnp.arange(4, dtype=jnp.int32)
    counts = jnp.where(slot_order == chosen, SHIFT_CAP, counts).astype(jnp.int32)
    upper_start = jax.random.randint(key_upper, (), 1, NY // 2 - counts[2] - counts[3] + 1).astype(jnp.int32)
    lower_start = jax.random.randint(key_lower, (), 1, NY // 2 - counts[1] - counts[0] + 2).astype(jnp.int32)
    ky_values = jnp.arange(NY, dtype=jnp.int32) - NY // 2
    upper_one = (ky_values >= upper_start) & (ky_values < upper_start + counts[2])
    upper_two = (ky_values >= upper_start + counts[2]) & (ky_values < upper_start + counts[2] + counts[3])
    lower_one = (ky_values <= -lower_start) & (ky_values > -lower_start - counts[1])
    lower_two = (ky_values <= -lower_start - counts[1]) & (ky_values > -lower_start - counts[1] - counts[0])
    offsets = (upper_one.astype(jnp.int32) + 2 * upper_two.astype(jnp.int32) - lower_one.astype(jnp.int32) - 2 * lower_two.astype(jnp.int32)).astype(jnp.int32)
    values = jnp.array([-2, -1, 1, 2], dtype=jnp.int32)
    chosen_value = jnp.sum(jnp.where(slot_order == chosen, values, 0)).astype(jnp.int32)
    coins = jax.random.randint(key_flag, (NY,), 0, 4).astype(jnp.int32)
    flag = jnp.where(offsets == chosen_value, 1, jnp.where(offsets != 0, (coins < 3).astype(jnp.int32), (coins < 2).astype(jnp.int32))).astype(jnp.int32)
    return (offsets, flag)


def draw_offsets(key, part):
    return remesh_plan(key)[0]


def draw_remesh_flag(key, part):
    return remesh_plan(key)[1]


def place_ends(result, stream_key, low, top_value):
    shape = result.shape
    place = [jax.random.randint(jax.random.fold_in(stream_key, axis), (), 0, shape[axis]) for axis in range(len(shape))]
    result = result.at[tuple(place)].set(low)
    longest = shape.index(max(shape))
    place[longest] = (place[longest] + 1) % shape[longest]
    return result.at[tuple(place)].set(top_value)


def level_of(own_key, extent, cuts, low, high):
    loudness, own = 1.0, jax.random.fold_in(own_key, 6)
    for axis_at, blocks in cuts:
        draws = jnp.exp(jax.random.uniform(jax.random.fold_in(own, axis_at), (blocks,), jnp.float32, low / len(cuts), high / len(cuts)))
        loudness = loudness * jnp.repeat(draws, extent[axis_at] // blocks).reshape([-1 if axis == axis_at else 1 for axis in range(len(extent))])
    return loudness


def normal_values(rng, shape, spread, most, cuts=(), kind=jnp.bfloat16):
    entries = jax.random.normal(rng, shape, jnp.float32) * spread
    if len(cuts) > 0:
        entries = level_of(rng, shape, cuts, -0.22, 0.18) * entries
    return jnp.clip(entries, min=-most, max=most).astype(kind)


def setup_inputs(seed: int = 0) -> dict:
    splits = jax.random.split(jax.random.key(seed), 6)
    return {
        "velocity": normal_values(splits[0], (3, 2, NZH, NX, NY), 1.0, 6.0, ((2, 8), (3, 16)), jnp.float32),
        "register": normal_values(splits[1], (3, 2, NZH, NX, NY), 1.0, 6.0, ((2, 8), (3, 16)), jnp.float32),
        "offsets": draw_offsets(jax.random.fold_in(splits[5], 71), 0),
        "remesh_flag": draw_remesh_flag(jax.random.fold_in(splits[5], 71), 0),
        "keep_blocks": place_ends((jax.random.randint(splits[4], (NBLK,), 0, 4) < 3).astype(jnp.int32), jax.random.fold_in(splits[4], 1), 0, 1),
    }


SHEAR_RATE = 40.0
SHEAR_TIME = 0.3
VISCOSITY = 0.0015
TIME_STEP = 0.008
REGISTER_WEIGHT = -153.0 / 128.0
UPDATE_WEIGHT = 8.0 / 15.0
PRODUCT_PAIRS = ((0, 0), (0, 1), (0, 2), (1, 1), (1, 2), (2, 2))
PAIR_LOOKUP = ((0, 1, 2), (1, 3, 4), (2, 4, 5))
OFFSET_VALUES = (-2, -1, 1, 2)
slab_rows = 32
kz_rows = 8

def phase_angles(contracted, produced, period):
    phase_turns = jnp.mod(contracted[:, None] * produced[None, :], period)
    return phase_turns.astype(jnp.float32) * (2.0 * math.pi / period)

def complex_table(contracted, produced, period, direction):
    angles = phase_angles(contracted, produced, period)
    cosine = jnp.cos(angles)
    sine_part = direction * jnp.sin(angles)
    upper_rows = jnp.stack([cosine, sine_part], axis=1)
    lower_rows = jnp.stack([-sine_part, cosine], axis=1)
    return jnp.stack([upper_rows, lower_rows], axis=0).astype(jnp.bfloat16)

def inverse_real_table(mode_list, points, period):
    angles = phase_angles(mode_list, points, period)
    weights = jnp.where(mode_list == 0, 1.0, 2.0).astype(jnp.float32)[:, None]
    return jnp.stack([weights * jnp.cos(angles), -weights * jnp.sin(angles)], axis=0).astype(jnp.bfloat16)

def forward_real_table(points, mode_list, period):
    angles = phase_angles(points, mode_list, period)
    return jnp.stack([jnp.cos(angles), -jnp.sin(angles)], axis=1).astype(jnp.bfloat16)

def tendency_update(spectra, velocity, register, kx_values, ky_values, kz_values):
    wave_x = kx_values[None, :, None] - SHEAR_TIME * ky_values[None, None, :]
    wave_y = ky_values[None, None, :]
    wave_z = kz_values[:, None, None]
    wave_list = (wave_x, wave_y, wave_z)
    squared = wave_x * wave_x + wave_y * wave_y + wave_z * wave_z
    inverse = 1.0 / jnp.maximum(squared, 1.0)
    advect_real = [sum((wave_list[source] * spectra[PAIR_LOOKUP[target][source], 1] for source in range(3))) for target in range(3)]
    advect_imag = [-sum((wave_list[source] * spectra[PAIR_LOOKUP[target][source], 0] for source in range(3))) for target in range(3)]
    diverge_real = sum((wave_list[target] * advect_real[target] for target in range(3)))
    diverge_imag = sum((wave_list[target] * advect_imag[target] for target in range(3)))
    pressure_lift = 2.0 * SHEAR_RATE * wave_y * inverse
    results = []
    for target in range(3):
        halves = []
        for half_index, advect, diverge in ((0, advect_real, diverge_real), (1, advect_imag, diverge_imag)):
            rate_value = advect[target] - wave_list[target] * diverge * inverse
            rate_value = rate_value + wave_list[target] * pressure_lift * velocity[0, half_index]
            rate_value = rate_value - VISCOSITY * squared * velocity[target, half_index]
            if target == 1:
                rate_value = rate_value - SHEAR_RATE * velocity[0, half_index]
            increment = REGISTER_WEIGHT * register[target, half_index] + TIME_STEP * rate_value
            halves.append(velocity[target, half_index] + UPDATE_WEIGHT * increment)
        results.append(jnp.stack(halves))
    return jnp.stack(results)

def contract(formula, left_operand, right_operand):
    return jnp.einsum(formula, left_operand.astype(jnp.float32), right_operand.astype(jnp.float32), precision=lax.Precision.HIGHEST)

def reference(velocity, register, offsets, remesh_flag, keep_blocks):
    inverse_scale = 1.0 / math.sqrt(NX * NY * NZ)
    forward_scale = math.sqrt(NX * NY * NZ) / (MX * MY * MZ)
    kx_all = jnp.arange(NX, dtype=jnp.int32) - NX // 2
    ky_all = jnp.arange(NY, dtype=jnp.int32) - NY // 2
    kz_all = jnp.arange(NZH, dtype=jnp.int32)
    x_points = jnp.arange(MX, dtype=jnp.int32)
    y_points = jnp.arange(MY, dtype=jnp.int32)
    z_points = jnp.arange(MZ, dtype=jnp.int32)
    y_inverse = complex_table(ky_all, y_points, MY, 1.0)
    x_inverse = complex_table(kx_all, x_points, MX, 1.0)
    z_inverse = inverse_real_table(kz_all, z_points, MZ)
    z_forward = forward_real_table(z_points, kz_all, MZ)
    x_forward = complex_table(x_points, kx_all, MX, -1.0)
    y_forward = complex_table(y_points, ky_all, MY, -1.0)
    collected = []
    for component in range(3):
        spectral = velocity[component].astype(jnp.bfloat16)
        along_y = contract('rlij,rjsq->slqi', spectral, y_inverse).astype(jnp.bfloat16)
        collected.append(contract('rlqi,risp->slqp', along_y, x_inverse).astype(jnp.bfloat16))
    grids = jnp.stack(collected)

    def slab_products(start):
        section = lax.dynamic_slice_in_dim(grids, start, slab_rows, 3)
        fields = contract('crlqp,rlz->cqpz', section, z_inverse) * inverse_scale
        products = jnp.stack([fields[left_factor] * fields[right_factor] for left_factor, right_factor in PRODUCT_PAIRS]).astype(jnp.bfloat16)
        modes_z = contract('eqpz,zsl->esqpl', products, z_forward).astype(jnp.bfloat16)
        return contract('erqpl,rpsi->esqil', modes_z, x_forward).astype(jnp.bfloat16)
    slabs = lax.map(slab_products, jnp.arange(MY // slab_rows, dtype=jnp.int32) * slab_rows)
    modes_x = jnp.moveaxis(slabs, 0, 2).reshape(6, 2, MY, NX, NZH)

    def kz_update(start):
        section = lax.dynamic_slice_in_dim(modes_x, start, kz_rows, 4)
        spectra = contract('erqil,rqsj->eslij', section, y_forward) * forward_scale
        velocity_part = lax.dynamic_slice_in_dim(velocity, start, kz_rows, 2)
        register_part = lax.dynamic_slice_in_dim(register, start, kz_rows, 2)
        kz_values = (start + jnp.arange(kz_rows, dtype=jnp.int32)).astype(jnp.float32)
        return tendency_update(spectra, velocity_part, register_part, kx_all.astype(jnp.float32), ky_all.astype(jnp.float32), kz_values)
    updates = lax.map(kz_update, jnp.arange(NZH // kz_rows, dtype=jnp.int32) * kz_rows)
    updated = jnp.moveaxis(updates, 0, 2).reshape(3, 2, NZH, NX, NY)
    moved_by = offsets * remesh_flag
    remeshed = updated * (moved_by == 0).astype(jnp.float32)
    for shift_by in OFFSET_VALUES:
        selected = updated * (moved_by == shift_by).astype(jnp.float32)
        amount = shift_by * KXB
        if amount > 0:
            selected = jnp.pad(selected[:, :, :, :NX - amount], ((0, 0), (0, 0), (0, 0), (amount, 0), (0, 0)))
        else:
            selected = jnp.pad(selected[:, :, :, -amount:], ((0, 0), (0, 0), (0, 0), (0, -amount), (0, 0)))
        remeshed = remeshed + selected
    block_keep = keep_blocks[jnp.arange(NX, dtype=jnp.int32) // KXB].astype(jnp.float32)
    return remeshed * block_keep[None, None, None, :, None]
```

```python
import functools
import math

import jax
import jax.numpy as jnp
import numpy as np
from jax import lax
from jax.experimental import pallas as pl
from jax.experimental.pallas import tpu as pltpu
from jax.sharding import PartitionSpec as P

NX = 512
NY = 256
NZ = 256
NZH = 128
MX = 768
MY = 384
MZ = 384
SHIFT_CAP = 32
ROWS = 8
COLS = 16
DEV = ROWS * COLS
YPD = MY // DEV
LKZ = NZH // ROWS
LKX = NX // COLS
HALF = LKZ // 2
PRODUCTS = 5

SHEAR_RATE = 40.0
SHEAR_TIME = 0.3
VISCOSITY = 0.0015
TIME_STEP = 0.008
REGISTER_WEIGHT = -153.0 / 128.0
UPDATE_WEIGHT = 8.0 / 15.0
OFFSET_VALUES = (-2, -1, 1, 2)
INVERSE_SCALE = 1.0 / math.sqrt(NX * NY * NZ)
FORWARD_SCALE = math.sqrt(NX * NY * NZ) / (MX * MY * MZ)

BF16 = jnp.bfloat16
F32 = jnp.float32


def angle_tables(first, second, period):
    turns = np.mod(first[:, None].astype(np.int64) * second[None, :].astype(np.int64), period)
    angles = turns.astype(np.float32) * np.float32(2.0 * math.pi / period)
    angles = angles.astype(np.float64)
    return np.cos(angles).astype(np.float32), np.sin(angles).astype(np.float32)


def y_table():
    cosine, sine = angle_tables(np.arange(MY), np.arange(NY) - NY // 2, MY)
    return jnp.asarray(np.concatenate([cosine, sine], axis=1).astype(BF16))


def z_tables():
    cosine, sine = angle_tables(np.arange(MZ), np.arange(NZH), MZ)
    weights = np.where(np.arange(NZH) == 0, 1.0, 2.0).astype(np.float32)[None, :]
    inverse = np.concatenate([weights * cosine, -weights * sine], axis=1).astype(BF16)
    forward = np.concatenate([cosine.T, -sine.T], axis=0).astype(BF16)
    return jnp.asarray(inverse), jnp.asarray(forward)


def x_factors():
    points = np.arange(MX)
    coarse = angle_tables(np.arange(COLS) * LKX - NX // 2, points, MX)
    fine = angle_tables(np.arange(LKX), points, MX)
    return [jnp.asarray(t) for t in coarse + fine]


def dot(a, b, dims):
    return lax.dot_general(a, b, (dims, ((), ())), preferred_element_type=F32)


def x_table_kernel(coarse_cos, coarse_sin, fine_cos, fine_sin, out):
    fc = fine_cos[...]
    fs = fine_sin[...]
    for col in range(COLS):
        a = coarse_cos[col : col + 1, :]
        b = coarse_sin[col : col + 1, :]
        real = (a * fc - b * fs).astype(BF16)
        imag_f = a * fs + b * fc
        base = col * 2 * LKX
        out[base : base + LKX, :MX] = real
        out[base : base + LKX, MX:] = imag_f.astype(BF16)
        out[base + LKX : base + 2 * LKX, :MX] = (-imag_f).astype(BF16)
        out[base + LKX : base + 2 * LKX, MX:] = real


def x_table():
    return pl.pallas_call(
        x_table_kernel,
        out_shape=jax.ShapeDtypeStruct((2 * NX, 2 * MX), BF16),
        name="x_table",
    )(*x_factors())


MSG_IN = YPD * 3 * HALF
GROUPS = 3 * HALF


def y_inverse_kernel(v_ref, table_ref, out_ref, rt_ref, scr_ref):
    c = pl.program_id(0)
    for lo in range(HALF):
        for hi in range(2):
            real = v_ref[0, 0, hi * HALF + lo].astype(BF16)
            imag = v_ref[0, 1, hi * HALF + lo].astype(BF16)
            base = (lo * 2 + hi) * 2 * LKX
            rt_ref[base : base + LKX, :NY] = real
            rt_ref[base : base + LKX, NY:] = -imag
            rt_ref[base + LKX : base + 2 * LKX, :NY] = imag
            rt_ref[base + LKX : base + 2 * LKX, NY:] = real
    for pair in range(HALF // 2):
        res = dot(table_ref[...], rt_ref[pair * 256 : (pair + 1) * 256, :], ((1,), (1,)))
        for y in range(YPD):
            for h in range(2):
                start = y * GROUPS + c * HALF + pair * 2 + h
                scr_ref[pl.ds(start, DEV, stride=MSG_IN), :] = res[
                    y * DEV : (y + 1) * DEV, h * 128 : (h + 1) * 128
                ]

    @pl.when(c == 2)
    def _():
        def pack(d, carry):
            rows = scr_ref[pl.ds(pl.multiple_of(d * 8 * MSG_IN, 8), 8 * MSG_IN), :]
            out_ref[pl.ds(d * 8, 8)] = rows.astype(BF16).reshape(8, MSG_IN, 128)
            return carry

        lax.fori_loop(0, DEV // 8, pack, 0)


def y_inverse(velocity):
    return pl.pallas_call(
        y_inverse_kernel,
        grid=(3,),
        in_specs=[
            pl.BlockSpec((1, 2, LKZ, LKX, NY), lambda c: (c, 0, 0, 0, 0)),
            pl.BlockSpec((MY, 2 * NY), lambda c: (0, 0)),
        ],
        out_specs=pl.BlockSpec((DEV, MSG_IN, 128), lambda c: (0, 0, 0)),
        out_shape=jax.ShapeDtypeStruct((DEV, MSG_IN, 128), BF16),
        scratch_shapes=[
            pltpu.VMEM((LKZ * 2 * LKX, 2 * NY), BF16),
            pltpu.VMEM((DEV * MSG_IN, 128), F32),
        ],
        compiler_params=pltpu.CompilerParams(vmem_limit_bytes=50 * 2**20),
        name="y_inverse",
    )(velocity, y_table())


MSG_OUT = YPD * PRODUCTS * HALF


def middle_kernel(m_ref, x_ref, zi_ref, zf_ref, o_ref, u_ref, w_ref, mz_ref):
    low3 = lax.broadcasted_iota(jnp.int32, (3 * HALF, 128), 1) < 64
    low5 = lax.broadcasted_iota(jnp.int32, (PRODUCTS * HALF, 128), 1) < 64

    def gather(r, carry):
        for cp in range(COLS // 2):
            a = m_ref[r * COLS + 2 * cp].astype(F32)
            b = m_ref[r * COLS + 2 * cp + 1].astype(F32)
            first = jnp.where(low3, a, pltpu.roll(b, 64, 1))
            second = jnp.where(low3, pltpu.roll(a, 64, 1), b)
            for c in range(3):
                rows = slice(c * HALF, (c + 1) * HALF)
                both = jnp.concatenate([first[rows], second[rows]], axis=0)
                start = pl.multiple_of(c * NZH + r * LKZ, LKZ)
                u_ref[pl.ds(start, LKZ), cp * 128 : (cp + 1) * 128] = both.astype(BF16)
        return carry

    lax.fori_loop(0, ROWS, gather, 0)

    for s in range(2):

        def x_inverse(n, carry, s=s):
            cols = pl.ds(pl.multiple_of(s * MX + n * 256, 256), 256)
            res = dot(u_ref[...], x_ref[:, cols], ((1,), (0,)))
            here = pl.ds(pl.multiple_of(n * 256, 256), 256)
            for c in range(3):
                start = c * 2 * NZH + s * NZH
                w_ref[start : start + NZH, here] = res[c * NZH : (c + 1) * NZH].astype(BF16)
            return carry

        lax.fori_loop(0, MX // 256, x_inverse, 0)

    def z_both(n, carry):
        here = pl.ds(pl.multiple_of(n * 256, 256), 256)
        there = pl.ds(pl.multiple_of(MX + n * 256, 256), 256)
        zi = zi_ref[...]
        zf = zf_ref[...]
        f0, f1, f2 = [
            dot(zi, w_ref[c * 2 * NZH : (c + 1) * 2 * NZH, here], ((1,), (0,))) * INVERSE_SCALE
            for c in range(3)
        ]
        last = f2 * f2
        products = (f0 * f0 - last, f0 * f1, f0 * f2, f1 * f1 - last, f1 * f2)
        for e, product in enumerate(products):
            res = dot(zf, product.astype(BF16), ((1,), (0,)))
            mz_ref[e * NZH : (e + 1) * NZH, here] = res[:NZH].astype(BF16)
            mz_ref[e * NZH : (e + 1) * NZH, there] = res[NZH:].astype(BF16)
        return carry

    lax.fori_loop(0, MX // 256, z_both, 0)

    def x_forward(n, carry):
        rows = pl.ds(pl.multiple_of(n * 256, 256), 256)
        res = dot(mz_ref[...], x_ref[rows, :], ((1,), (1,)))
        for half in range(2):
            for r in range(ROWS):
                lo, hi = [
                    jnp.concatenate(
                        [
                            res[
                                e * NZH + r * LKZ + h * HALF : e * NZH + r * LKZ + (h + 1) * HALF,
                                half * 128 : (half + 1) * 128,
                            ]
                            for e in range(PRODUCTS)
                        ],
                        axis=0,
                    )
                    for h in range(2)
                ]
                first = jnp.where(low5, lo, pltpu.roll(hi, 64, 1))
                second = jnp.where(low5, pltpu.roll(lo, 64, 1), hi)
                dest = r * COLS + 4 * n + 2 * half
                o_ref[dest] = first.astype(BF16)
                o_ref[dest + 1] = second.astype(BF16)
        return carry

    lax.fori_loop(0, NX * 2 // 256, x_forward, 0)


def middle(messages, table):
    zi, zf = z_tables()
    return pl.pallas_call(
        middle_kernel,
        grid=(YPD,),
        in_specs=[
            pl.BlockSpec((DEV, 3 * HALF, 128), lambda y: (0, y, 0)),
            pl.BlockSpec((2 * NX, 2 * MX), lambda y: (0, 0)),
            pl.BlockSpec((MZ, 2 * NZH), lambda y: (0, 0)),
            pl.BlockSpec((2 * NZH, MZ), lambda y: (0, 0)),
        ],
        out_specs=pl.BlockSpec((DEV, PRODUCTS * HALF, 128), lambda y: (0, y, 0)),
        out_shape=jax.ShapeDtypeStruct((DEV, MSG_OUT, 128), BF16),
        scratch_shapes=[
            pltpu.VMEM((3 * NZH, 2 * NX), BF16),
            pltpu.VMEM((6 * NZH, MX), BF16),
            pltpu.VMEM((PRODUCTS * NZH, 2 * MX), BF16),
        ],
        compiler_params=pltpu.CompilerParams(vmem_limit_bytes=50 * 2**20),
        name="middle",
    )(messages, table, zi, zf)


PACK = 2 * 6 * LKX


def update_kernel(
    scal_ref, g_ref, table_ref, v_ref, reg_ref, place_ref, stay_ref, base_ref, p0, p1, p2, p3, scr_ref
):
    lo = pl.program_id(0)

    @pl.when(lo == 0)
    def _():
        def unpack(d, carry):
            rows = g_ref[pl.ds(d * 8, 8)].astype(F32).reshape(8 * MSG_OUT, 128)
            scr_ref[pl.ds(pl.multiple_of(d * 8 * MSG_OUT, 8), 8 * MSG_OUT), :] = rows
            return carry

        lax.fori_loop(0, DEV // 8, unpack, 0)

    table = table_ref[...]
    spectra = []
    for e in range(PRODUCTS):
        parts = [
            scr_ref[
                pl.ds(y * PRODUCTS * HALF + e * HALF + lo, DEV, stride=MSG_OUT), :
            ].astype(BF16)
            for y in range(YPD)
        ]
        spectra.append(dot(jnp.concatenate(parts, axis=0), table, ((0,), (0,))))

    kx0 = scal_ref[0]
    kz0 = scal_ref[1]
    shape = (LKX, NY)
    k2 = (lax.broadcasted_iota(jnp.int32, shape, 1) - NY // 2).astype(F32)
    k1 = lax.broadcasted_iota(jnp.int32, shape, 0).astype(F32) + kx0 - SHEAR_TIME * k2
    stay = stay_ref[...]
    moving = []
    for hi in range(2):
        k3 = kz0 + (lo + hi * HALF).astype(F32)
        waves = (k1, k2, k3)
        squared = k1 * k1 + k2 * k2 + k3 * k3
        inverse = 1.0 / jnp.maximum(squared, 1.0)
        real = []
        imag = []
        for p in spectra:
            top = p[hi * 2 * LKX : hi * 2 * LKX + LKX]
            bottom = p[hi * 2 * LKX + LKX : (hi + 1) * 2 * LKX]
            real.append((top[:, :NY] + bottom[:, NY:]) * FORWARD_SCALE)
            imag.append((bottom[:, :NY] - top[:, NY:]) * FORWARD_SCALE)

        def rows_of(t):
            return (
                k1 * t[0] + k2 * t[1] + k3 * t[2],
                k1 * t[1] + k2 * t[3] + k3 * t[4],
                k1 * t[2] + k2 * t[4],
            )

        advect_parts = (rows_of(imag), tuple(-a for a in rows_of(real)))
        lift = 2.0 * SHEAR_RATE * k2 * inverse
        for half in range(2):
            advect = advect_parts[half]
            diverge = k1 * advect[0] + k2 * advect[1] + k3 * advect[2]
            first = v_ref[0, half, hi, 0]
            common = lift * first - diverge * inverse
            for m in range(3):
                velocity = v_ref[m, half, hi, 0]
                rate = advect[m] + waves[m] * common
                rate = rate - VISCOSITY * squared * velocity
                if m == 1:
                    rate = rate - SHEAR_RATE * first
                increment = REGISTER_WEIGHT * reg_ref[m, half, hi, 0] + TIME_STEP * rate
                updated = velocity + UPDATE_WEIGHT * increment
                base_ref[m, half, hi, 0] = updated * stay
                moving.append(updated.astype(BF16))
    packed = dot(place_ref[...], jnp.concatenate(moving, axis=0), ((1,), (1,))).astype(BF16)
    for position, ref in enumerate((p0, p1, p2, p3)):
        ref[...] = packed[position * SHIFT_CAP : (position + 1) * SHIFT_CAP]


FIELD = (3, 2, 2, HALF, LKX, NY)
FIELD_BLOCK = pl.BlockSpec((3, 2, 2, 1, LKX, NY), lambda lo: (0, 0, 0, lo, 0, 0))
MOVE_BLOCK = pl.BlockSpec((SHIFT_CAP, PACK), lambda lo: (0, lo))


def update(scalars, gathered, velocity, register, place, stay):
    return pl.pallas_call(
        update_kernel,
        grid=(HALF,),
        in_specs=[
            pl.BlockSpec(memory_space=pltpu.SMEM),
            pl.BlockSpec((DEV, MSG_OUT, 128), lambda lo: (0, 0, 0)),
            pl.BlockSpec((MY, 2 * NY), lambda lo: (0, 0)),
            FIELD_BLOCK,
            FIELD_BLOCK,
            pl.BlockSpec((4 * SHIFT_CAP, NY), lambda lo: (0, 0)),
            pl.BlockSpec((1, NY), lambda lo: (0, 0)),
        ],
        out_specs=[FIELD_BLOCK] + [MOVE_BLOCK] * 4,
        out_shape=[jax.ShapeDtypeStruct(FIELD, F32)]
        + [jax.ShapeDtypeStruct((SHIFT_CAP, HALF * PACK), BF16)] * 4,
        scratch_shapes=[pltpu.VMEM((DEV * MSG_OUT, 128), F32)],
        compiler_params=pltpu.CompilerParams(vmem_limit_bytes=50 * 2**20),
        name="update",
    )(scalars, gathered, y_table(), velocity.reshape(FIELD), register.reshape(FIELD), place, stay)


def settle_kernel(scal_ref, base_ref, a0, a1, a2, a3, place_ref, out_ref):
    arrived = jnp.concatenate([a0[...], a1[...], a2[...], a3[...]], axis=0)
    moved = dot(arrived, place_ref[...], ((0,), (0,)))
    keep = scal_ref[2]
    for hi in range(2):
        for m in range(3):
            for half in range(2):
                start = (hi * 6 + half * 3 + m) * LKX
                out_ref[m, half, hi, 0] = (
                    base_ref[m, half, hi, 0] + moved[start : start + LKX]
                ) * keep


def settle(scalars, base, arrivals, place):
    return pl.pallas_call(
        settle_kernel,
        grid=(HALF,),
        in_specs=[pl.BlockSpec(memory_space=pltpu.SMEM), FIELD_BLOCK]
        + [MOVE_BLOCK] * 4
        + [pl.BlockSpec((4 * SHIFT_CAP, NY), lambda lo: (0, 0))],
        out_specs=FIELD_BLOCK,
        out_shape=jax.ShapeDtypeStruct(FIELD, F32),
        name="settle",
    )(scalars, base, *arrivals, place)


def from_behind(block, axis, distance):
    devices = range(COLS)
    route = [(i - distance, i) for i in devices if i - distance in devices]
    return lax.ppermute(block, axis, route)


def local(velocity, register, offsets, remesh_flag, keep_blocks):
    row_index = lax.axis_index("row")
    col_index = lax.axis_index("col")
    moved_by = offsets * remesh_flag
    marked = jnp.stack([moved_by == value for value in OFFSET_VALUES])
    order = jnp.arange(NY, dtype=jnp.int32)
    upto = (order[:, None] <= order[None, :]).astype(BF16)
    ranked = jnp.dot(marked.astype(BF16), upto, preferred_element_type=F32).astype(jnp.int32) - 1
    slots = jnp.arange(SHIFT_CAP, dtype=jnp.int32)
    place = (marked[:, None, :] & (ranked[:, None, :] == slots[None, :, None])).astype(BF16)
    place = place.reshape(4 * SHIFT_CAP, NY)
    stay = (moved_by == 0).astype(F32).reshape(1, NY)
    keep_here = jnp.sum(
        jnp.where(jnp.arange(COLS, dtype=jnp.int32) == col_index, keep_blocks, 0)
    ).astype(F32)
    scalars = jnp.stack(
        [
            (col_index * LKX - NX // 2).astype(F32),
            (row_index * LKZ).astype(F32),
            keep_here,
        ]
    )

    outgoing = y_inverse(velocity)
    table = x_table()
    messages = lax.all_to_all(outgoing, ("row", "col"), split_axis=0, concat_axis=0, tiled=True)
    returning = middle(messages, table)
    gathered = lax.all_to_all(returning, ("row", "col"), split_axis=0, concat_axis=0, tiled=True)
    base, *packed = update(scalars, gathered, velocity, register, place, stay)
    arrivals = [
        from_behind(block, "col", value) for block, value in zip(packed, OFFSET_VALUES)
    ]
    result = settle(scalars, base, arrivals, place)
    return result.reshape(velocity.shape)


def solution(mesh):
    placed = (P(None, None, "row", "col", None), P(None, None, "row", "col", None), P(), P(), P())
    return jax.shard_map(
        local,
        mesh=mesh,
        in_specs=placed,
        out_specs=P(None, None, "row", "col", None),
        check_vma=False,
    )
```

```python
import functools
import math

import jax
import jax.numpy as jnp
import numpy as np
from jax import lax
from jax.experimental import pallas as pl
from jax.experimental.pallas import tpu as pltpu
from jax.sharding import PartitionSpec as P

NX = 512
NY = 256
NZ = 256
NZH = 128
MX = 768
MY = 384
MZ = 384
SHIFT_CAP = 32
ROWS = 8
COLS = 16
DEV = ROWS * COLS
YPD = MY // DEV
LKZ = NZH // ROWS
LKX = NX // COLS
HALF = LKZ // 2
PRODUCTS = 5

SHEAR_RATE = 40.0
SHEAR_TIME = 0.3
VISCOSITY = 0.0015
TIME_STEP = 0.008
REGISTER_WEIGHT = -153.0 / 128.0
UPDATE_WEIGHT = 8.0 / 15.0
OFFSET_VALUES = (-2, -1, 1, 2)
INVERSE_SCALE = 1.0 / math.sqrt(NX * NY * NZ)
FORWARD_SCALE = math.sqrt(NX * NY * NZ) / (MX * MY * MZ)

BF16 = jnp.bfloat16
F32 = jnp.float32


def angle_tables(first, second, period):
    turns = np.mod(first[:, None].astype(np.int64) * second[None, :].astype(np.int64), period)
    angles = turns.astype(np.float32) * np.float32(2.0 * math.pi / period)
    angles = angles.astype(np.float64)
    return np.cos(angles).astype(np.float32), np.sin(angles).astype(np.float32)


def y_table():
    cosine, sine = angle_tables(np.arange(MY), np.arange(NY) - NY // 2, MY)
    return jnp.asarray(np.concatenate([cosine, sine], axis=1).astype(BF16))


def z_tables():
    slots = np.arange(MZ // 2)
    partners = np.where(slots == 0, MZ // 2, MZ - slots)
    modes = np.arange(NZH)
    cosine, sine = angle_tables(np.concatenate([slots, partners]), modes, MZ)
    weights = np.where(modes == 0, 1.0, 2.0).astype(np.float32)[None, :]
    inverse = np.concatenate([weights * cosine, -weights * sine], axis=1).astype(BF16)
    even = (modes % 2 == 0).astype(np.float32)
    real = np.zeros((NZH, MZ // 2 + 16), np.float32)
    real[:, : MZ // 2] = cosine[: MZ // 2].T
    real[:, 0] = even
    real[:, MZ // 2] = 1.0 - even
    imag = -sine[: MZ // 2].T
    return [jnp.asarray(t) for t in (inverse, real.astype(BF16), imag.astype(BF16))]


def x_factors():
    points = np.arange(MX // 2)
    coarse = angle_tables(np.arange(COLS) * LKX - NX // 2, points, MX)
    fine = angle_tables(np.arange(LKX), points, MX)
    return [jnp.asarray(t) for t in coarse + fine]


def dot(a, b, dims):
    return lax.dot_general(a, b, (dims, ((), ())), preferred_element_type=F32)


XN = MX // 256


def x_table_kernel(coarse_cos, coarse_sin, fine_cos, fine_sin, out):
    shape = (LKX, 128)
    first = lax.broadcasted_iota(jnp.int32, shape, 1) == 0
    odd = lax.rem(lax.broadcasted_iota(jnp.int32, shape, 0), 2).astype(F32)
    for n in range(XN):
        here = slice(n * 128, (n + 1) * 128)
        fc = fine_cos[:, here]
        fs = fine_sin[:, here]
        for col in range(COLS):
            a = coarse_cos[col : col + 1, here]
            b = coarse_sin[col : col + 1, here]
            cosine = a * fc - b * fs
            sine = a * fs + b * fc
            if n == 0:
                cosine = jnp.where(first, 1.0 - odd, cosine)
                sine = jnp.where(first, odd, sine)
            rows = slice(col * LKX, (col + 1) * LKX)
            out[rows, n * 256 : n * 256 + 128] = cosine.astype(BF16)
            out[rows, n * 256 + 128 : (n + 1) * 256] = sine.astype(BF16)


def x_table():
    return pl.pallas_call(
        x_table_kernel,
        out_shape=jax.ShapeDtypeStruct((NX, MX), BF16),
        compiler_params=pltpu.CompilerParams(vmem_limit_bytes=12 * 2**20),
        name="x_table",
    )(*x_factors())


MSG_IN = YPD * 3 * HALF
GROUPS = YPD * HALF


def y_inverse_kernel(v_ref, table_ref, out_ref, rt_ref, scr_ref):
    for lo in range(HALF):
        for hi in range(2):
            real = v_ref[0, 0, hi * HALF + lo].astype(BF16)
            imag = v_ref[0, 1, hi * HALF + lo].astype(BF16)
            base = (lo * 2 + hi) * 2 * LKX
            rt_ref[base : base + LKX, :NY] = real
            rt_ref[base : base + LKX, NY:] = -imag
            rt_ref[base + LKX : base + 2 * LKX, :NY] = imag
            rt_ref[base + LKX : base + 2 * LKX, NY:] = real
    for pair in range(HALF // 2):
        res = dot(table_ref[...], rt_ref[pair * 256 : (pair + 1) * 256, :], ((1,), (1,)))
        for y in range(YPD):
            for h in range(2):
                start = y * HALF + pair * 2 + h
                scr_ref[pl.ds(start, DEV, stride=GROUPS), :] = res[
                    y * DEV : (y + 1) * DEV, h * 128 : (h + 1) * 128
                ]

    def pack(d, carry):
        rows = scr_ref[pl.ds(pl.multiple_of(d * 8 * GROUPS, 8), 8 * GROUPS), :]
        out_ref[pl.ds(d * 8, 8)] = rows.astype(BF16).reshape(8, GROUPS, 128)
        return carry

    lax.fori_loop(0, DEV // 8, pack, 0)


def y_inverse(velocity):
    return pl.pallas_call(
        y_inverse_kernel,
        grid=(3,),
        in_specs=[
            pl.BlockSpec((1, 2, LKZ, LKX, NY), lambda c: (c, 0, 0, 0, 0)),
            pl.BlockSpec((MY, 2 * NY), lambda c: (0, 0)),
        ],
        out_specs=pl.BlockSpec((DEV, GROUPS, 128), lambda c: (0, c, 0)),
        out_shape=pltpu.HBM((DEV, MSG_IN, 128), BF16),
        scratch_shapes=[
            pltpu.VMEM((LKZ * 2 * LKX, 2 * NY), BF16),
            pltpu.VMEM((DEV * GROUPS, 128), F32),
        ],
        compiler_params=pltpu.CompilerParams(vmem_limit_bytes=60 * 2**20),
        name="y_inverse",
    )(velocity, y_table())


MSG_OUT = YPD * PRODUCTS * HALF


def exchange4(a, b, c, d, low, even):
    ac0 = jnp.where(low, a, pltpu.roll(c, 64, 1))
    ac1 = jnp.where(low, pltpu.roll(a, 64, 1), c)
    bd0 = jnp.where(low, b, pltpu.roll(d, 64, 1))
    bd1 = jnp.where(low, pltpu.roll(b, 64, 1), d)
    return (
        jnp.where(even, ac0, pltpu.roll(bd0, 32, 1)),
        jnp.where(even, pltpu.roll(ac0, 96, 1), bd0),
        jnp.where(even, ac1, pltpu.roll(bd1, 32, 1)),
        jnp.where(even, pltpu.roll(ac1, 96, 1), bd1),
    )


def lane_masks(rows):
    lanes = lax.broadcasted_iota(jnp.int32, (rows, 128), 1)
    return lanes < 64, lax.rem(lanes, 64) < 32


def middle_kernel(m_ref, x_ref, zi_ref, zr_ref, zm_ref, o_ref, u_ref, f_ref):
    y = pl.program_id(0)
    rows_of_y = [
        pl.ds(pl.multiple_of(c * GROUPS + y * HALF, HALF), HALF) for c in range(3)
    ]
    masks = lane_masks(3 * HALF)
    for r in range(ROWS):
        for cg in range(COLS // 4):
            four = [
                jnp.concatenate(
                    [
                        m_ref[r * COLS + 4 * cg + q, here, :].astype(F32) for here in rows_of_y
                    ],
                    axis=0,
                )
                for q in range(4)
            ]
            parts = exchange4(*four, *masks)
            for s in range(2):
                for c in range(3):
                    rows = slice(c * HALF, (c + 1) * HALF)
                    both = jnp.concatenate([parts[s][rows], parts[2 + s][rows]], axis=0)
                    start = (s * 3 + c) * NZH + r * LKZ
                    u_ref[start : start + LKZ, cg * 128 : (cg + 1) * 128] = both.astype(BF16)

    zi = zi_ref[...]
    zr = zr_ref[...]
    zm = zm_ref[...]
    first = lax.broadcasted_iota(jnp.int32, (NZH, 128), 1) == 0
    half = MZ // 2
    for n in range(XN):
        here = slice(n * 256, (n + 1) * 256)
        res = dot(u_ref[...], x_ref[:, here], ((1,), (0,)))
        fields = []
        for c in range(3):
            top = slice(c * NZH, (c + 1) * NZH)
            bottom = slice((3 + c) * NZH, (4 + c) * NZH)
            cr, sr = res[top, :128], res[top, 128:]
            ci, si = res[bottom, :128], res[bottom, 128:]
            x1, x2 = si, sr
            if n == 0:
                x1 = jnp.where(first, -sr, si)
                x2 = jnp.where(first, si, sr)
            modes = jnp.concatenate(
                [
                    jnp.concatenate([cr - x1, cr + x1], axis=1),
                    jnp.concatenate([ci + x2, ci - x2], axis=1),
                ],
                axis=0,
            ).astype(BF16)
            fields.append(dot(zi, modes, ((1,), (0,))))
        f0, f1, f2 = fields
        last = f2 * f2
        products = (f0 * f0 - last, f0 * f1, f0 * f2, f1 * f1 - last, f1 * f2)
        for e, product in enumerate(products):
            even = (product[:half] + product[half:]).astype(BF16)
            odd = (product[:half] - product[half:]).astype(BF16)
            mr = dot(zr, jnp.concatenate([even, odd[:16]], axis=0), ((1,), (0,)))
            mi = dot(zm, odd, ((1,), (0,)))
            er, orr = mr[:, :128] + mr[:, 128:], mr[:, :128] - mr[:, 128:]
            ei, oi = mi[:, :128] + mi[:, 128:], mi[:, :128] - mi[:, 128:]
            x1, x2 = oi, -orr
            if n == 0:
                x1 = jnp.where(first, orr, oi)
                x2 = jnp.where(first, oi, -orr)
            top = slice(e * NZH, (e + 1) * NZH)
            bottom = slice((PRODUCTS + e) * NZH, (PRODUCTS + e + 1) * NZH)
            f_ref[top, here] = jnp.concatenate([er, x1], axis=1).astype(BF16)
            f_ref[bottom, here] = jnp.concatenate([ei, x2], axis=1).astype(BF16)

    masks = lane_masks(PRODUCTS * HALF)
    for m in range(NX // 256):
        res = dot(f_ref[...], x_ref[m * 256 : (m + 1) * 256, :], ((1,), (1,)))
        for side in range(2):
            for r in range(ROWS):
                four = []
                for hi in range(2):
                    for s in range(2):
                        pieces = []
                        for e in range(PRODUCTS):
                            start = (s * PRODUCTS + e) * NZH + r * LKZ + hi * HALF
                            pieces.append(
                                res[start : start + HALF, side * 128 : (side + 1) * 128]
                            )
                        four.append(jnp.concatenate(pieces, axis=0))
                parts = exchange4(*four, *masks)
                for q in range(4):
                    o_ref[r * COLS + 4 * (2 * m + side) + q] = parts[q].astype(BF16)


def middle(messages, table):
    return pl.pallas_call(
        middle_kernel,
        grid=(YPD,),
        in_specs=[
            pl.BlockSpec((DEV, MSG_IN, 128), lambda y: (0, 0, 0)),
            pl.BlockSpec((NX, MX), lambda y: (0, 0)),
            pl.BlockSpec((MZ, 2 * NZH), lambda y: (0, 0)),
            pl.BlockSpec((NZH, MZ // 2 + 16), lambda y: (0, 0)),
            pl.BlockSpec((NZH, MZ // 2), lambda y: (0, 0)),
        ],
        out_specs=pl.BlockSpec((DEV, PRODUCTS * HALF, 128), lambda y: (0, y, 0)),
        out_shape=pltpu.HBM((DEV, MSG_OUT, 128), BF16),
        scratch_shapes=[
            pltpu.VMEM((6 * NZH, NX), BF16),
            pltpu.VMEM((2 * PRODUCTS * NZH, MX), BF16),
        ],
        compiler_params=pltpu.CompilerParams(vmem_limit_bytes=26 * 2**20),
        name="middle",
    )(messages, table, *z_tables())


PACK = 2 * 6 * LKX
PARTS = 4
FIELD = (3, 2, 2, HALF, LKX, NY)


def field_block(per):
    return pl.BlockSpec((3, 2, 2, per, LKX, NY), lambda k: (0, 0, 0, k, 0, 0))


def move_block(per):
    return pl.BlockSpec((SHIFT_CAP, per * PACK), lambda k: (0, k))


LINEAR_PER = 4
UPDATE_PER = 2
SETTLE_PER = 4


def wave_numbers(scal_ref, lo, hi):
    shape = (LKX, NY)
    k2 = (lax.broadcasted_iota(jnp.int32, shape, 1) - NY // 2).astype(F32)
    k1 = lax.broadcasted_iota(jnp.int32, shape, 0).astype(F32) + scal_ref[0] - SHEAR_TIME * k2
    k3 = scal_ref[1] + (lo + hi * HALF).astype(F32)
    squared = k1 * k1 + k2 * k2 + k3 * k3
    return k1, k2, k3, squared, 1.0 / jnp.maximum(squared, 1.0)


def linear_kernel(scal_ref, v_ref, reg_ref, out_ref):
    for u, hi in ((u, hi) for u in range(LINEAR_PER) for hi in range(2)):
        lo = pl.program_id(0) * LINEAR_PER + u
        k1, k2, k3, squared, inverse = wave_numbers(scal_ref, lo, hi)
        lift = 2.0 * SHEAR_RATE * k2 * inverse
        for half in range(2):
            first = v_ref[0, half, hi, u]
            lifted = lift * first
            for m, wave in enumerate((k1, k2, k3)):
                velocity = v_ref[m, half, hi, u]
                rate = wave * lifted - VISCOSITY * squared * velocity
                if m == 1:
                    rate = rate - SHEAR_RATE * first
                increment = REGISTER_WEIGHT * reg_ref[m, half, hi, u] + TIME_STEP * rate
                out_ref[m, half, hi, u] = velocity + UPDATE_WEIGHT * increment


def linear_part(scalars, velocity, register):
    return pl.pallas_call(
        linear_kernel,
        grid=(HALF // LINEAR_PER,),
        in_specs=[pl.BlockSpec(memory_space=pltpu.SMEM), field_block(LINEAR_PER), field_block(LINEAR_PER)],
        out_specs=field_block(LINEAR_PER),
        out_shape=pltpu.HBM(FIELD, F32),
        compiler_params=pltpu.CompilerParams(vmem_limit_bytes=60 * 2**20),
        name="linear",
    )(scalars, velocity.reshape(FIELD), register.reshape(FIELD))


def update_kernel(
    scal_ref, g_hbm, table_ref, lin_ref, place_ref, stay_ref, base_ref, p0, p1, p2, p3, scr_ref,
    g_ref, sems,
):
    step = pl.program_id(0)

    @pl.when(step == 0)
    def _():
        copies = []
        for part in range(PARTS):
            here = pl.ds(part * (DEV // PARTS), DEV // PARTS)
            copies.append(pltpu.make_async_copy(g_hbm.at[here], g_ref.at[here], sems.at[part]))
            copies[-1].start()

        def unpack(d, carry):
            rows = g_ref[pl.ds(d * 8, 8)].astype(F32).reshape(8 * MSG_OUT, 128)
            scr_ref[pl.ds(pl.multiple_of(d * 8 * MSG_OUT, 8), 8 * MSG_OUT), :] = rows
            return carry

        share = DEV // 8 // PARTS
        for part in range(PARTS):
            copies[part].wait()
            lax.fori_loop(part * share, (part + 1) * share, unpack, 0)

    table = table_ref[...]
    stay = stay_ref[...]
    weight = UPDATE_WEIGHT * TIME_STEP * FORWARD_SCALE * INVERSE_SCALE * INVERSE_SCALE
    for u in range(UPDATE_PER):
        lo = step * UPDATE_PER + u
        spectra = []
        for e in range(PRODUCTS):
            parts = [
                scr_ref[
                    pl.ds(y * PRODUCTS * HALF + e * HALF + lo, DEV, stride=MSG_OUT), :
                ].astype(BF16)
                for y in range(YPD)
            ]
            spectra.append(dot(jnp.concatenate(parts, axis=0), table, ((0,), (0,))))

        moving = []
        for hi in range(2):
            k1, k2, k3, squared, inverse = wave_numbers(scal_ref, lo, hi)
            real = []
            imag = []
            for p in spectra:
                top = p[hi * 2 * LKX : hi * 2 * LKX + LKX]
                bottom = p[hi * 2 * LKX + LKX : (hi + 1) * 2 * LKX]
                real.append(top[:, :NY] + bottom[:, NY:])
                imag.append(bottom[:, :NY] - top[:, NY:])
            for half, t, sign in ((0, imag, weight), (1, real, -weight)):
                stress = (
                    k1 * t[0] + k2 * t[1] + k3 * t[2],
                    k1 * t[1] + k2 * t[3] + k3 * t[4],
                    k1 * t[2] + k2 * t[4],
                )
                pressure = (k1 * stress[0] + k2 * stress[1] + k3 * stress[2]) * inverse
                for m, wave in enumerate((k1, k2, k3)):
                    updated = lin_ref[m, half, hi, u] + sign * (stress[m] - wave * pressure)
                    base_ref[m, half, hi, u] = updated * stay
                    moving.append(updated.astype(BF16))
        packed = dot(place_ref[...], jnp.concatenate(moving, axis=0), ((1,), (1,))).astype(BF16)
        for position, ref in enumerate((p0, p1, p2, p3)):
            ref[:, u * PACK : (u + 1) * PACK] = packed[position * SHIFT_CAP : (position + 1) * SHIFT_CAP]


def update(scalars, gathered, linear, place, stay):
    return pl.pallas_call(
        update_kernel,
        grid=(HALF // UPDATE_PER,),
        in_specs=[
            pl.BlockSpec(memory_space=pltpu.SMEM),
            pl.BlockSpec(memory_space=pl.ANY),
            pl.BlockSpec((MY, 2 * NY), lambda lo: (0, 0)),
            field_block(UPDATE_PER),
            pl.BlockSpec((4 * SHIFT_CAP, NY), lambda lo: (0, 0)),
            pl.BlockSpec((1, NY), lambda lo: (0, 0)),
        ],
        out_specs=[field_block(UPDATE_PER)] + [move_block(UPDATE_PER)] * 4,
        out_shape=[jax.ShapeDtypeStruct(FIELD, F32)]
        + [jax.ShapeDtypeStruct((SHIFT_CAP, HALF * PACK), BF16)] * 4,
        scratch_shapes=[
            pltpu.VMEM((DEV * MSG_OUT, 128), F32),
            pltpu.VMEM((DEV, MSG_OUT, 128), BF16),
            pltpu.SemaphoreType.DMA((PARTS,)),
        ],
        compiler_params=pltpu.CompilerParams(vmem_limit_bytes=60 * 2**20),
        name="update",
    )(scalars, gathered, y_table(), linear, place, stay)


def settle_kernel(scal_ref, base_ref, a0, a1, a2, a3, place_ref, out_ref):
    arrived = jnp.concatenate([a0[...], a1[...], a2[...], a3[...]], axis=0)
    moved = dot(arrived, place_ref[...], ((0,), (0,)))
    keep = scal_ref[2]
    for u, hi in ((u, hi) for u in range(SETTLE_PER) for hi in range(2)):
        for m in range(3):
            for half in range(2):
                start = u * PACK + (hi * 6 + half * 3 + m) * LKX
                out_ref[m, half, hi, u] = (
                    base_ref[m, half, hi, u] + moved[start : start + LKX]
                ) * keep


def settle(scalars, base, arrivals, place):
    return pl.pallas_call(
        settle_kernel,
        grid=(HALF // SETTLE_PER,),
        in_specs=[pl.BlockSpec(memory_space=pltpu.SMEM), field_block(SETTLE_PER)]
        + [move_block(SETTLE_PER)] * 4
        + [pl.BlockSpec((4 * SHIFT_CAP, NY), lambda lo: (0, 0))],
        out_specs=field_block(SETTLE_PER),
        out_shape=jax.ShapeDtypeStruct(FIELD, F32),
        compiler_params=pltpu.CompilerParams(vmem_limit_bytes=16 * 2**20),
        name="settle",
    )(scalars, base, *arrivals, place)


def from_behind(block, axis, distance):
    return lax.ppermute(block, axis, [((i - distance) % COLS, i) for i in range(COLS)])


def local(velocity, register, offsets, remesh_flag, keep_blocks):
    row_index = lax.axis_index("row")
    col_index = lax.axis_index("col")
    moved_by = offsets * remesh_flag
    marked = jnp.stack([moved_by == value for value in OFFSET_VALUES])
    order = jnp.arange(NY, dtype=jnp.int32)
    upto = (order[:, None] <= order[None, :]).astype(BF16)
    ranked = jnp.dot(marked.astype(BF16), upto, preferred_element_type=F32).astype(jnp.int32) - 1
    slots = jnp.arange(SHIFT_CAP, dtype=jnp.int32)
    place = (marked[:, None, :] & (ranked[:, None, :] == slots[None, :, None])).astype(BF16)
    place = place.reshape(4 * SHIFT_CAP, NY)
    stay = (moved_by == 0).astype(F32).reshape(1, NY)
    keep_here = jnp.sum(
        jnp.where(jnp.arange(COLS, dtype=jnp.int32) == col_index, keep_blocks, 0)
    ).astype(F32)
    scalars = jnp.stack(
        [
            (col_index * LKX - NX // 2).astype(F32),
            (row_index * LKZ).astype(F32),
            keep_here,
        ]
    )

    outgoing = y_inverse(velocity)
    table = x_table()
    messages = lax.all_to_all(outgoing, ("row", "col"), split_axis=0, concat_axis=0, tiled=True)
    returning = middle(messages, table)
    gathered = lax.all_to_all(returning, ("row", "col"), split_axis=0, concat_axis=0, tiled=True)
    linear = linear_part(scalars, velocity, register)
    base, *packed = update(scalars, gathered, linear, place, stay)
    arrivals = [
        from_behind(block, "col", value) for block, value in zip(packed, OFFSET_VALUES)
    ]
    sources = [col_index - value for value in OFFSET_VALUES]
    inside = jnp.stack([(source >= 0) & (source < COLS) for source in sources])
    taking = jnp.repeat(inside, SHIFT_CAP)[:, None].astype(BF16) * place
    result = settle(scalars, base, arrivals, taking)
    return result.reshape(velocity.shape)


def solution(mesh):
    placed = (P(None, None, "row", "col", None), P(None, None, "row", "col", None), P(), P(), P())
    return jax.shard_map(
        local,
        mesh=mesh,
        in_specs=placed,
        out_specs=P(None, None, "row", "col", None),
        check_vma=False,
    )
```

```python
import functools
import math

import jax
import jax.numpy as jnp
import numpy as np
from jax import lax
from jax.experimental import pallas as pl
from jax.experimental.pallas import tpu as pltpu
from jax.sharding import PartitionSpec as P

NX = 512
NY = 256
NZ = 256
NZH = 128
MX = 768
MY = 384
MZ = 384
SHIFT_CAP = 32
ROWS = 8
COLS = 16
DEV = ROWS * COLS
YPD = MY // DEV
LKZ = NZH // ROWS
LKX = NX // COLS
HALF = LKZ // 2
PRODUCTS = 5

SHEAR_RATE = 40.0
SHEAR_TIME = 0.3
VISCOSITY = 0.0015
TIME_STEP = 0.008
REGISTER_WEIGHT = -153.0 / 128.0
UPDATE_WEIGHT = 8.0 / 15.0
OFFSET_VALUES = (-2, -1, 1, 2)
INVERSE_SCALE = 1.0 / math.sqrt(NX * NY * NZ)
FORWARD_SCALE = math.sqrt(NX * NY * NZ) / (MX * MY * MZ)

BF16 = jnp.bfloat16
F32 = jnp.float32


def angle_tables(first, second, period):
    turns = np.mod(first[:, None].astype(np.int64) * second[None, :].astype(np.int64), period)
    angles = turns.astype(np.float32) * np.float32(2.0 * math.pi / period)
    angles = angles.astype(np.float64)
    return np.cos(angles).astype(np.float32), np.sin(angles).astype(np.float32)


def y_table():
    cosine, sine = angle_tables(np.arange(MY), np.arange(NY) - NY // 2, MY)
    return jnp.asarray(np.concatenate([cosine, sine], axis=1).astype(BF16))


def z_tables():
    slots = np.arange(MZ // 2)
    partners = np.where(slots == 0, MZ // 2, MZ - slots)
    modes = np.arange(NZH)
    cosine, sine = angle_tables(np.concatenate([slots, partners]), modes, MZ)
    weights = np.where(modes == 0, 1.0, 2.0).astype(np.float32)[None, :]
    inverse = np.concatenate([weights * cosine, -weights * sine], axis=1).astype(BF16)
    even = (modes % 2 == 0).astype(np.float32)
    real = np.zeros((NZH, MZ // 2 + 16), np.float32)
    real[:, : MZ // 2] = cosine[: MZ // 2].T
    real[:, 0] = even
    real[:, MZ // 2] = 1.0 - even
    imag = -sine[: MZ // 2].T
    return [jnp.asarray(t) for t in (inverse, real.astype(BF16), imag.astype(BF16))]


def x_factors():
    points = np.arange(MX // 2)
    coarse = angle_tables(np.arange(COLS) * LKX - NX // 2, points, MX)
    fine = angle_tables(np.arange(LKX), points, MX)
    return [jnp.asarray(t) for t in coarse + fine]


def dot(a, b, dims):
    return lax.dot_general(a, b, (dims, ((), ())), preferred_element_type=F32)


XN = MX // 256


def x_table_kernel(coarse_cos, coarse_sin, fine_cos, fine_sin, out):
    shape = (LKX, 128)
    first = lax.broadcasted_iota(jnp.int32, shape, 1) == 0
    odd = lax.rem(lax.broadcasted_iota(jnp.int32, shape, 0), 2).astype(F32)
    for n in range(XN):
        here = slice(n * 128, (n + 1) * 128)
        fc = fine_cos[:, here]
        fs = fine_sin[:, here]
        for col in range(COLS):
            a = coarse_cos[col : col + 1, here]
            b = coarse_sin[col : col + 1, here]
            cosine = a * fc - b * fs
            sine = a * fs + b * fc
            if n == 0:
                cosine = jnp.where(first, 1.0 - odd, cosine)
                sine = jnp.where(first, odd, sine)
            rows = slice(col * LKX, (col + 1) * LKX)
            out[rows, n * 256 : n * 256 + 128] = cosine.astype(BF16)
            out[rows, n * 256 + 128 : (n + 1) * 256] = sine.astype(BF16)


def x_table():
    return pl.pallas_call(
        x_table_kernel,
        out_shape=jax.ShapeDtypeStruct((NX, MX), BF16),
        compiler_params=pltpu.CompilerParams(vmem_limit_bytes=12 * 2**20),
        name="x_table",
    )(*x_factors())


MSG_IN = YPD * 3 * HALF
GROUPS = YPD * HALF


def y_inverse_kernel(v_ref, table_ref, out_ref, rt_ref, scr_ref):
    for lo in range(HALF):
        for hi in range(2):
            real = v_ref[0, 0, hi * HALF + lo].astype(BF16)
            imag = v_ref[0, 1, hi * HALF + lo].astype(BF16)
            base = (lo * 2 + hi) * 2 * LKX
            rt_ref[base : base + LKX, :NY] = real
            rt_ref[base : base + LKX, NY:] = -imag
            rt_ref[base + LKX : base + 2 * LKX, :NY] = imag
            rt_ref[base + LKX : base + 2 * LKX, NY:] = real
    for pair in range(HALF // 2):
        res = dot(table_ref[...], rt_ref[pair * 256 : (pair + 1) * 256, :], ((1,), (1,)))
        for y in range(YPD):
            for h in range(2):
                start = y * HALF + pair * 2 + h
                scr_ref[pl.ds(start, DEV, stride=GROUPS), :] = res[
                    y * DEV : (y + 1) * DEV, h * 128 : (h + 1) * 128
                ]

    def pack(d, carry):
        rows = scr_ref[pl.ds(pl.multiple_of(d * 8 * GROUPS, 8), 8 * GROUPS), :]
        out_ref[pl.ds(d * 8, 8)] = rows.astype(BF16).reshape(8, GROUPS, 128)
        return carry

    lax.fori_loop(0, DEV // 8, pack, 0)


def y_inverse(velocity):
    return pl.pallas_call(
        y_inverse_kernel,
        grid=(3,),
        in_specs=[
            pl.BlockSpec((1, 2, LKZ, LKX, NY), lambda c: (c, 0, 0, 0, 0)),
            pl.BlockSpec((MY, 2 * NY), lambda c: (0, 0)),
        ],
        out_specs=pl.BlockSpec((DEV, GROUPS, 128), lambda c: (0, c, 0)),
        out_shape=pltpu.HBM((DEV, MSG_IN, 128), BF16),
        scratch_shapes=[
            pltpu.VMEM((LKZ * 2 * LKX, 2 * NY), BF16),
            pltpu.VMEM((DEV * GROUPS, 128), F32),
        ],
        compiler_params=pltpu.CompilerParams(vmem_limit_bytes=60 * 2**20),
        name="y_inverse",
    )(velocity, y_table())


MSG_OUT = YPD * PRODUCTS * HALF


def exchange4(a, b, c, d, low, even):
    ac0 = jnp.where(low, a, pltpu.roll(c, 64, 1))
    ac1 = jnp.where(low, pltpu.roll(a, 64, 1), c)
    bd0 = jnp.where(low, b, pltpu.roll(d, 64, 1))
    bd1 = jnp.where(low, pltpu.roll(b, 64, 1), d)
    return (
        jnp.where(even, ac0, pltpu.roll(bd0, 32, 1)),
        jnp.where(even, pltpu.roll(ac0, 96, 1), bd0),
        jnp.where(even, ac1, pltpu.roll(bd1, 32, 1)),
        jnp.where(even, pltpu.roll(ac1, 96, 1), bd1),
    )


def lane_masks(rows):
    lanes = lax.broadcasted_iota(jnp.int32, (rows, 128), 1)
    return lanes < 64, lax.rem(lanes, 64) < 32


def middle_kernel(
    m_ref, x_ref, zi_ref, zr_ref, zm_ref, o_ref, u_ref, f_ref, w_ref, d_ref, t_ref
):
    y = pl.program_id(0)
    rows_of_y = [
        pl.ds(pl.multiple_of(c * GROUPS + y * HALF, HALF), HALF) for c in range(3)
    ]
    masks = lane_masks(3 * HALF)
    for r in range(ROWS):
        for cg in range(COLS // 4):
            four = [
                jnp.concatenate(
                    [
                        m_ref[r * COLS + 4 * cg + q, here, :].astype(F32) for here in rows_of_y
                    ],
                    axis=0,
                )
                for q in range(4)
            ]
            parts = exchange4(*four, *masks)
            for s in range(2):
                for c in range(3):
                    rows = slice(c * HALF, (c + 1) * HALF)
                    both = jnp.concatenate([parts[s][rows], parts[2 + s][rows]], axis=0)
                    start = (c * 2 + s) * NZH + r * LKZ
                    u_ref[start : start + LKZ, cg * 128 : (cg + 1) * 128] = both.astype(BF16)

    zi = zi_ref[...]
    zr = zr_ref[...]
    zm = zm_ref[...]
    first = lax.broadcasted_iota(jnp.int32, (LKZ, 128), 1) == 0
    half = MZ // 2
    for c in range(3):
        res = dot(u_ref[c * 2 * NZH : (c + 1) * 2 * NZH], x_ref[...], ((1,), (0,)))
        for n in range(XN):
            cos_at = slice(n * 256, n * 256 + 128)
            sin_at = slice(n * 256 + 128, (n + 1) * 256)
            for k in range(0, NZH, LKZ):
                top = slice(k, k + LKZ)
                bottom = slice(NZH + k, NZH + k + LKZ)
                cr, sr = res[top, cos_at], res[top, sin_at]
                ci, si = res[bottom, cos_at], res[bottom, sin_at]
                x1, x2 = si, sr
                if n == 0:
                    x1 = jnp.where(first, -sr, si)
                    x2 = jnp.where(first, si, sr)
                w_ref[c, top, cos_at] = (cr - x1).astype(BF16)
                w_ref[c, top, sin_at] = (cr + x1).astype(BF16)
                w_ref[c, bottom, cos_at] = (ci + x2).astype(BF16)
                w_ref[c, bottom, sin_at] = (ci - x2).astype(BF16)
        d_ref[c] = dot(zi, w_ref[c], ((1,), (0,)))
    for n in range(XN):
        here = slice(n * 256, (n + 1) * 256)
        for k in range(0, half, LKZ):
            pair = []
            for start in (k, half + k):
                f0, f1, f2 = [d_ref[c, start : start + LKZ, here] for c in range(3)]
                last = f2 * f2
                pair.append((f0 * f0 - last, f0 * f1, f0 * f2, f1 * f1 - last, f1 * f2))
            for e in range(PRODUCTS):
                t_ref[e, k : k + LKZ, here] = (pair[0][e] + pair[1][e]).astype(BF16)
                t_ref[e, half + k : half + k + LKZ, here] = (pair[0][e] - pair[1][e]).astype(BF16)
    for e in range(PRODUCTS):
        mr = dot(zr, t_ref[e, : half + LKZ], ((1,), (0,)))
        mi = dot(zm, t_ref[e, half:], ((1,), (0,)))
        for n in range(XN):
            cos_at = slice(n * 256, n * 256 + 128)
            sin_at = slice(n * 256 + 128, (n + 1) * 256)
            for k in range(0, NZH, LKZ):
                rows = slice(k, k + LKZ)
                er, orr = mr[rows, cos_at] + mr[rows, sin_at], mr[rows, cos_at] - mr[rows, sin_at]
                ei, oi = mi[rows, cos_at] + mi[rows, sin_at], mi[rows, cos_at] - mi[rows, sin_at]
                x1, x2 = oi, -orr
                if n == 0:
                    x1 = jnp.where(first, orr, oi)
                    x2 = jnp.where(first, oi, -orr)
                top = slice(e * NZH + k, e * NZH + k + LKZ)
                bottom = slice((PRODUCTS + e) * NZH + k, (PRODUCTS + e) * NZH + k + LKZ)
                f_ref[top, cos_at] = er.astype(BF16)
                f_ref[top, sin_at] = x1.astype(BF16)
                f_ref[bottom, cos_at] = ei.astype(BF16)
                f_ref[bottom, sin_at] = x2.astype(BF16)

    masks = lane_masks(PRODUCTS * HALF)
    for m in range(NX // 256):
        res = dot(f_ref[...], x_ref[m * 256 : (m + 1) * 256, :], ((1,), (1,)))
        for side in range(2):
            for r in range(ROWS):
                four = []
                for hi in range(2):
                    for s in range(2):
                        pieces = []
                        for e in range(PRODUCTS):
                            start = (s * PRODUCTS + e) * NZH + r * LKZ + hi * HALF
                            pieces.append(
                                res[start : start + HALF, side * 128 : (side + 1) * 128]
                            )
                        four.append(jnp.concatenate(pieces, axis=0))
                parts = exchange4(*four, *masks)
                for q in range(4):
                    o_ref[r * COLS + 4 * (2 * m + side) + q] = parts[q].astype(BF16)


def middle(messages, table):
    return pl.pallas_call(
        middle_kernel,
        grid=(YPD,),
        in_specs=[
            pl.BlockSpec((DEV, MSG_IN, 128), lambda y: (0, 0, 0)),
            pl.BlockSpec((NX, MX), lambda y: (0, 0)),
            pl.BlockSpec((MZ, 2 * NZH), lambda y: (0, 0)),
            pl.BlockSpec((NZH, MZ // 2 + 16), lambda y: (0, 0)),
            pl.BlockSpec((NZH, MZ // 2), lambda y: (0, 0)),
        ],
        out_specs=pl.BlockSpec((DEV, PRODUCTS * HALF, 128), lambda y: (0, y, 0)),
        out_shape=pltpu.HBM((DEV, MSG_OUT, 128), BF16),
        scratch_shapes=[
            pltpu.VMEM((6 * NZH, NX), BF16),
            pltpu.VMEM((2 * PRODUCTS * NZH, MX), BF16),
            pltpu.VMEM((3, 2 * NZH, MX), BF16),
            pltpu.VMEM((3, MZ, MX), F32),
            pltpu.VMEM((PRODUCTS, MZ, MX), BF16),
        ],
        compiler_params=pltpu.CompilerParams(vmem_limit_bytes=26 * 2**20),
        name="middle",
    )(messages, table, *z_tables())


PACK = 2 * 6 * LKX
PARTS = 4
FIELD = (3, 2, 2, HALF, LKX, NY)


def field_block(per):
    return pl.BlockSpec((3, 2, 2, per, LKX, NY), lambda k: (0, 0, 0, k, 0, 0))


def slab_block(per):
    return pl.BlockSpec((1, 3, 2, 2, per, LKX, NY), lambda k: (0, 0, 0, 0, k, 0, 0))


def move_block(per):
    return pl.BlockSpec((SHIFT_CAP, per * PACK), lambda k: (0, k))


SLABS = 8
LINEAR_PER = 4
UPDATE_PER = 2
SETTLE_PER = 4


def wave_numbers(scal_ref, lo, hi):
    shape = (LKX, NY)
    k2 = (lax.broadcasted_iota(jnp.int32, shape, 1) - NY // 2).astype(F32)
    k1 = lax.broadcasted_iota(jnp.int32, shape, 0).astype(F32) + scal_ref[0] - SHEAR_TIME * k2
    k3 = scal_ref[1] + (lo + hi * HALF).astype(F32)
    squared = k1 * k1 + k2 * k2 + k3 * k3
    return k1, k2, k3, squared, 1.0 / jnp.maximum(squared, 1.0)


def linear_kernel(scal_ref, v_ref, reg_ref, out_ref):
    for u, hi in ((u, hi) for u in range(LINEAR_PER) for hi in range(2)):
        lo = pl.program_id(0) * LINEAR_PER + u
        k1, k2, k3, squared, inverse = wave_numbers(scal_ref, lo, hi)
        lift = 2.0 * SHEAR_RATE * k2 * inverse
        for half in range(2):
            first = v_ref[0, half, hi, u]
            lifted = lift * first
            for m, wave in enumerate((k1, k2, k3)):
                velocity = v_ref[m, half, hi, u]
                rate = wave * lifted - VISCOSITY * squared * velocity
                if m == 1:
                    rate = rate - SHEAR_RATE * first
                increment = REGISTER_WEIGHT * reg_ref[m, half, hi, u] + TIME_STEP * rate
                out_ref[0, m, half, hi, u] = velocity + UPDATE_WEIGHT * increment


def linear_part(scalars, velocity, register):
    return pl.pallas_call(
        linear_kernel,
        grid=(HALF // LINEAR_PER,),
        in_specs=[pl.BlockSpec(memory_space=pltpu.SMEM), field_block(LINEAR_PER), field_block(LINEAR_PER)],
        out_specs=slab_block(LINEAR_PER),
        out_shape=pltpu.HBM((SLABS,) + FIELD, F32),
        compiler_params=pltpu.CompilerParams(vmem_limit_bytes=60 * 2**20),
        name="linear",
    )(scalars, velocity.reshape(FIELD), register.reshape(FIELD))


def update_kernel(
    scal_ref, g_hbm, table_ref, lin_ref, place_ref, stay_ref, base_ref, p0, p1, p2, p3, scr_ref,
    g_ref, sems,
):
    step = pl.program_id(0)

    @pl.when(step == 0)
    def _():
        copies = []
        for part in range(PARTS):
            here = pl.ds(part * (DEV // PARTS), DEV // PARTS)
            copies.append(pltpu.make_async_copy(g_hbm.at[here], g_ref.at[here], sems.at[part]))
            copies[-1].start()

        def unpack(d, carry):
            rows = g_ref[pl.ds(d * 8, 8)].astype(F32).reshape(8 * MSG_OUT, 128)
            scr_ref[pl.ds(pl.multiple_of(d * 8 * MSG_OUT, 8), 8 * MSG_OUT), :] = rows
            return carry

        share = DEV // 8 // PARTS
        for part in range(PARTS):
            copies[part].wait()
            lax.fori_loop(part * share, (part + 1) * share, unpack, 0)

    table = table_ref[...]
    stay = stay_ref[...]
    weight = UPDATE_WEIGHT * TIME_STEP * FORWARD_SCALE * INVERSE_SCALE * INVERSE_SCALE
    for u in range(UPDATE_PER):
        lo = step * UPDATE_PER + u
        spectra = []
        for e in range(PRODUCTS):
            parts = [
                scr_ref[
                    pl.ds(y * PRODUCTS * HALF + e * HALF + lo, DEV, stride=MSG_OUT), :
                ].astype(BF16)
                for y in range(YPD)
            ]
            spectra.append(dot(jnp.concatenate(parts, axis=0), table, ((0,), (0,))))

        moving = []
        for hi in range(2):
            k1, k2, k3, squared, inverse = wave_numbers(scal_ref, lo, hi)
            real = []
            imag = []
            for p in spectra:
                top = p[hi * 2 * LKX : hi * 2 * LKX + LKX]
                bottom = p[hi * 2 * LKX + LKX : (hi + 1) * 2 * LKX]
                real.append(top[:, :NY] + bottom[:, NY:])
                imag.append(bottom[:, :NY] - top[:, NY:])
            for half, t, sign in ((0, imag, weight), (1, real, -weight)):
                stress = (
                    k1 * t[0] + k2 * t[1] + k3 * t[2],
                    k1 * t[1] + k2 * t[3] + k3 * t[4],
                    k1 * t[2] + k2 * t[4],
                )
                pressure = (k1 * stress[0] + k2 * stress[1] + k3 * stress[2]) * inverse
                for m, wave in enumerate((k1, k2, k3)):
                    updated = lin_ref[0, m, half, hi, u] + sign * (stress[m] - wave * pressure)
                    base_ref[m, half, hi, u] = updated * stay
                    moving.append(updated.astype(BF16))
        packed = dot(place_ref[...], jnp.concatenate(moving, axis=0), ((1,), (1,))).astype(BF16)
        for position, ref in enumerate((p0, p1, p2, p3)):
            ref[:, u * PACK : (u + 1) * PACK] = packed[position * SHIFT_CAP : (position + 1) * SHIFT_CAP]


def update(scalars, gathered, linear, place, stay):
    return pl.pallas_call(
        update_kernel,
        grid=(HALF // UPDATE_PER,),
        in_specs=[
            pl.BlockSpec(memory_space=pltpu.SMEM),
            pl.BlockSpec(memory_space=pl.ANY),
            pl.BlockSpec((MY, 2 * NY), lambda lo: (0, 0)),
            slab_block(UPDATE_PER),
            pl.BlockSpec((4 * SHIFT_CAP, NY), lambda lo: (0, 0)),
            pl.BlockSpec((1, NY), lambda lo: (0, 0)),
        ],
        out_specs=[field_block(UPDATE_PER)] + [move_block(UPDATE_PER)] * 4,
        out_shape=[jax.ShapeDtypeStruct(FIELD, F32)]
        + [jax.ShapeDtypeStruct((SHIFT_CAP, HALF * PACK), BF16)] * 4,
        scratch_shapes=[
            pltpu.VMEM((DEV * MSG_OUT, 128), F32),
            pltpu.VMEM((DEV, MSG_OUT, 128), BF16),
            pltpu.SemaphoreType.DMA((PARTS,)),
        ],
        compiler_params=pltpu.CompilerParams(vmem_limit_bytes=44 * 2**20),
        name="update",
    )(scalars, gathered, y_table(), linear, place, stay)


def settle_kernel(scal_ref, base_ref, a0, a1, a2, a3, place_ref, out_ref):
    arrived = jnp.concatenate([a0[...], a1[...], a2[...], a3[...]], axis=0)
    moved = dot(arrived, place_ref[...], ((0,), (0,)))
    keep = scal_ref[2]
    for u, hi in ((u, hi) for u in range(SETTLE_PER) for hi in range(2)):
        for m in range(3):
            for half in range(2):
                start = u * PACK + (hi * 6 + half * 3 + m) * LKX
                out_ref[m, half, hi, u] = (
                    base_ref[m, half, hi, u] + moved[start : start + LKX]
                ) * keep


def settle(scalars, base, arrivals, place):
    return pl.pallas_call(
        settle_kernel,
        grid=(HALF // SETTLE_PER,),
        in_specs=[pl.BlockSpec(memory_space=pltpu.SMEM), field_block(SETTLE_PER)]
        + [move_block(SETTLE_PER)] * 4
        + [pl.BlockSpec((4 * SHIFT_CAP, NY), lambda lo: (0, 0))],
        out_specs=field_block(SETTLE_PER),
        out_shape=jax.ShapeDtypeStruct(FIELD, F32),
        compiler_params=pltpu.CompilerParams(vmem_limit_bytes=16 * 2**20),
        name="settle",
    )(scalars, base, *arrivals, place)


def from_behind(block, axis, distance):
    return lax.ppermute(block, axis, [((i - distance) % COLS, i) for i in range(COLS)])


def local(velocity, register, offsets, remesh_flag, keep_blocks):
    row_index = lax.axis_index("row")
    col_index = lax.axis_index("col")
    moved_by = offsets * remesh_flag
    marked = jnp.stack([moved_by == value for value in OFFSET_VALUES])
    order = jnp.arange(NY, dtype=jnp.int32)
    upto = (order[:, None] <= order[None, :]).astype(BF16)
    ranked = jnp.dot(marked.astype(BF16), upto, preferred_element_type=F32).astype(jnp.int32) - 1
    slots = jnp.arange(SHIFT_CAP, dtype=jnp.int32)
    place = (marked[:, None, :] & (ranked[:, None, :] == slots[None, :, None])).astype(BF16)
    place = place.reshape(4 * SHIFT_CAP, NY)
    stay = (moved_by == 0).astype(F32).reshape(1, NY)
    keep_here = jnp.sum(
        jnp.where(jnp.arange(COLS, dtype=jnp.int32) == col_index, keep_blocks, 0)
    ).astype(F32)
    scalars = jnp.stack(
        [
            (col_index * LKX - NX // 2).astype(F32),
            (row_index * LKZ).astype(F32),
            keep_here,
        ]
    )

    outgoing = y_inverse(velocity)
    table = x_table()
    messages = lax.all_to_all(outgoing, ("row", "col"), split_axis=0, concat_axis=0, tiled=True)
    returning = middle(messages, table)
    gathered = lax.all_to_all(returning, ("row", "col"), split_axis=0, concat_axis=0, tiled=True)
    linear = linear_part(scalars, velocity, register)
    base, *packed = update(scalars, gathered, linear, place, stay)
    arrivals = [
        from_behind(block, "col", value) for block, value in zip(packed, OFFSET_VALUES)
    ]
    sources = [col_index - value for value in OFFSET_VALUES]
    inside = jnp.stack([(source >= 0) & (source < COLS) for source in sources])
    taking = jnp.repeat(inside, SHIFT_CAP)[:, None].astype(BF16) * place
    result = settle(scalars, base, arrivals, taking)
    return result.reshape(velocity.shape)


def solution(mesh):
    placed = (P(None, None, "row", "col", None), P(None, None, "row", "col", None), P(), P(), P())
    return jax.shard_map(
        local,
        mesh=mesh,
        in_specs=placed,
        out_specs=P(None, None, "row", "col", None),
        check_vma=False,
    )
```

```python
import functools
import math

import jax
import jax.numpy as jnp
import numpy as np
from jax import lax
from jax.experimental import pallas as pl
from jax.experimental.pallas import tpu as pltpu
from jax.sharding import PartitionSpec as P

NX = 512
NY = 256
NZ = 256
NZH = 128
MX = 768
MY = 384
MZ = 384
SHIFT_CAP = 32
ROWS = 8
COLS = 16
DEV = ROWS * COLS
YPD = MY // DEV
LKZ = NZH // ROWS
LKX = NX // COLS
HALF = LKZ // 2
PRODUCTS = 5

SHEAR_RATE = 40.0
SHEAR_TIME = 0.3
VISCOSITY = 0.0015
TIME_STEP = 0.008
REGISTER_WEIGHT = -153.0 / 128.0
UPDATE_WEIGHT = 8.0 / 15.0
OFFSET_VALUES = (-2, -1, 1, 2)
INVERSE_SCALE = 1.0 / math.sqrt(NX * NY * NZ)
FORWARD_SCALE = math.sqrt(NX * NY * NZ) / (MX * MY * MZ)

BF16 = jnp.bfloat16
F32 = jnp.float32


def angle_tables(first, second, period):
    turns = np.mod(first[:, None].astype(np.int64) * second[None, :].astype(np.int64), period)
    angles = turns.astype(np.float32) * np.float32(2.0 * math.pi / period)
    angles = angles.astype(np.float64)
    return np.cos(angles).astype(np.float32), np.sin(angles).astype(np.float32)


def y_table():
    cosine, sine = angle_tables(np.arange(MY), np.arange(NY) - NY // 2, MY)
    return jnp.asarray(np.concatenate([cosine, sine], axis=1).astype(BF16))


def z_tables():
    slots = np.arange(MZ // 2)
    partners = np.where(slots == 0, MZ // 2, MZ - slots)
    modes = np.arange(NZH)
    cosine, sine = angle_tables(np.concatenate([slots, partners]), modes, MZ)
    weights = np.where(modes == 0, 1.0, 2.0).astype(np.float32)[None, :]
    inverse = np.concatenate([weights * cosine, -weights * sine], axis=1).astype(BF16)
    even = (modes % 2 == 0).astype(np.float32)
    real = np.zeros((NZH, MZ // 2 + 16), np.float32)
    real[:, : MZ // 2] = cosine[: MZ // 2].T
    real[:, 0] = even
    real[:, MZ // 2] = 1.0 - even
    imag = -sine[: MZ // 2].T
    return [jnp.asarray(t) for t in (inverse, real.astype(BF16), imag.astype(BF16))]


def x_factors():
    points = np.arange(MX // 2)
    coarse = angle_tables(np.arange(COLS) * LKX - NX // 2, points, MX)
    fine = angle_tables(np.arange(LKX), points, MX)
    return [jnp.asarray(t) for t in coarse + fine]


def dot(a, b, dims):
    return lax.dot_general(a, b, (dims, ((), ())), preferred_element_type=F32)


XN = MX // 256


def x_table_kernel(coarse_cos, coarse_sin, fine_cos, fine_sin, out):
    shape = (LKX, 128)
    first = lax.broadcasted_iota(jnp.int32, shape, 1) == 0
    odd = lax.rem(lax.broadcasted_iota(jnp.int32, shape, 0), 2).astype(F32)
    for n in range(XN):
        here = slice(n * 128, (n + 1) * 128)
        fc = fine_cos[:, here]
        fs = fine_sin[:, here]
        for col in range(COLS):
            a = coarse_cos[col : col + 1, here]
            b = coarse_sin[col : col + 1, here]
            cosine = a * fc - b * fs
            sine = a * fs + b * fc
            if n == 0:
                cosine = jnp.where(first, 1.0 - odd, cosine)
                sine = jnp.where(first, odd, sine)
            rows = slice(col * LKX, (col + 1) * LKX)
            out[rows, n * 256 : n * 256 + 128] = cosine.astype(BF16)
            out[rows, n * 256 + 128 : (n + 1) * 256] = sine.astype(BF16)


def x_table():
    return pl.pallas_call(
        x_table_kernel,
        out_shape=jax.ShapeDtypeStruct((NX, MX), BF16),
        compiler_params=pltpu.CompilerParams(vmem_limit_bytes=12 * 2**20),
        name="x_table",
    )(*x_factors())


MSG_IN = YPD * 3 * HALF
GROUPS = YPD * HALF


def y_inverse_kernel(v_hbm, t_hbm, out_hbm, v_ref, t_ref, rt_ref, scr_ref, o_ref, sems):
    loads = [pltpu.make_async_copy(v_hbm.at[c], v_ref.at[c], sems.at[c]) for c in range(3)]
    load_table = pltpu.make_async_copy(t_hbm, t_ref, sems.at[3])
    loads[0].start()
    load_table.start()
    loads[1].start()
    loads[2].start()
    stores = []
    for c in range(3):
        rt = rt_ref.at[c % 2]
        scr = scr_ref.at[c % 2]
        loads[c].wait()
        for lo in range(HALF):
            for hi in range(2):
                real = v_ref[c, 0, hi * HALF + lo].astype(BF16)
                imag = v_ref[c, 1, hi * HALF + lo].astype(BF16)
                base = (lo * 2 + hi) * 2 * LKX
                rt[base : base + LKX, :NY] = real
                rt[base : base + LKX, NY:] = -imag
                rt[base + LKX : base + 2 * LKX, :NY] = imag
                rt[base + LKX : base + 2 * LKX, NY:] = real
        if c == 0:
            load_table.wait()
        for quad in range(2):
            res = dot(t_ref[...], rt[quad * 512 : (quad + 1) * 512, :], ((1,), (1,)))
            for y in range(YPD):
                for h in range(4):
                    start = y * HALF + quad * 4 + h
                    scr[pl.ds(start, DEV, stride=GROUPS), :] = res[
                        y * DEV : (y + 1) * DEV, h * 128 : (h + 1) * 128
                    ]

        def pack(d, carry, c=c, scr=scr):
            rows = scr[pl.ds(pl.multiple_of(d * 16 * GROUPS, 8), 16 * GROUPS), :]
            o_ref[c, pl.ds(d * 16, 16)] = rows.astype(BF16).reshape(16, GROUPS, 128)
            return carry

        lax.fori_loop(0, DEV // 16, pack, 0)
        here = pl.ds(c * GROUPS, GROUPS)
        stores.append(pltpu.make_async_copy(o_ref.at[c], out_hbm.at[:, here], sems.at[4 + c]))
        stores[-1].start()
    for store in stores:
        store.wait()


def y_inverse(velocity):
    return pl.pallas_call(
        y_inverse_kernel,
        in_specs=[pl.BlockSpec(memory_space=pltpu.HBM)] * 2,
        out_specs=pl.BlockSpec(memory_space=pltpu.HBM),
        out_shape=pltpu.HBM((DEV, MSG_IN, 128), BF16),
        scratch_shapes=[
            pltpu.VMEM((3, 2, LKZ, LKX, NY), F32),
            pltpu.VMEM((MY, 2 * NY), BF16),
            pltpu.VMEM((2, LKZ * 2 * LKX, 2 * NY), BF16),
            pltpu.VMEM((2, DEV * GROUPS, 128), F32),
            pltpu.VMEM((3, DEV, GROUPS, 128), BF16),
            pltpu.SemaphoreType.DMA((7,)),
        ],
        compiler_params=pltpu.CompilerParams(vmem_limit_bytes=60 * 2**20),
        name="y_inverse",
    )(velocity, y_table())


MSG_OUT = YPD * PRODUCTS * HALF


def exchange4(a, b, c, d, low, even):
    ac0 = jnp.where(low, a, pltpu.roll(c, 64, 1))
    ac1 = jnp.where(low, pltpu.roll(a, 64, 1), c)
    bd0 = jnp.where(low, b, pltpu.roll(d, 64, 1))
    bd1 = jnp.where(low, pltpu.roll(b, 64, 1), d)
    return (
        jnp.where(even, ac0, pltpu.roll(bd0, 32, 1)),
        jnp.where(even, pltpu.roll(ac0, 96, 1), bd0),
        jnp.where(even, ac1, pltpu.roll(bd1, 32, 1)),
        jnp.where(even, pltpu.roll(ac1, 96, 1), bd1),
    )


def lane_masks(rows):
    lanes = lax.broadcasted_iota(jnp.int32, (rows, 128), 1)
    return lanes < 64, lax.rem(lanes, 64) < 32


def middle_kernel(
    m_ref, x_ref, zi_ref, zr_ref, zm_ref, o_ref, u_ref, f_ref, w_ref, d_ref, t_ref
):
    y = pl.program_id(0)
    rows_of_y = [
        pl.ds(pl.multiple_of(c * GROUPS + y * HALF, HALF), HALF) for c in range(3)
    ]
    masks = lane_masks(3 * HALF)
    for r in range(ROWS):
        for cg in range(COLS // 4):
            four = [
                jnp.concatenate(
                    [
                        m_ref[r * COLS + 4 * cg + q, here, :].astype(F32) for here in rows_of_y
                    ],
                    axis=0,
                )
                for q in range(4)
            ]
            parts = exchange4(*four, *masks)
            for s in range(2):
                for c in range(3):
                    rows = slice(c * HALF, (c + 1) * HALF)
                    both = jnp.concatenate([parts[s][rows], parts[2 + s][rows]], axis=0)
                    start = (c * 2 + s) * NZH + r * LKZ
                    u_ref[start : start + LKZ, cg * 128 : (cg + 1) * 128] = both.astype(BF16)

    zi = zi_ref[...]
    zr = zr_ref[...]
    zm = zm_ref[...]
    first = lax.broadcasted_iota(jnp.int32, (LKZ, 128), 1) == 0
    half = MZ // 2
    for c in range(3):
        res = dot(u_ref[c * 2 * NZH : (c + 1) * 2 * NZH], x_ref[...], ((1,), (0,)))
        for n in range(XN):
            cos_at = slice(n * 256, n * 256 + 128)
            sin_at = slice(n * 256 + 128, (n + 1) * 256)
            for k in range(0, NZH, LKZ):
                top = slice(k, k + LKZ)
                bottom = slice(NZH + k, NZH + k + LKZ)
                cr, sr = res[top, cos_at], res[top, sin_at]
                ci, si = res[bottom, cos_at], res[bottom, sin_at]
                x1, x2 = si, sr
                if n == 0:
                    x1 = jnp.where(first, -sr, si)
                    x2 = jnp.where(first, si, sr)
                w_ref[c, top, cos_at] = (cr - x1).astype(BF16)
                w_ref[c, top, sin_at] = (cr + x1).astype(BF16)
                w_ref[c, bottom, cos_at] = (ci + x2).astype(BF16)
                w_ref[c, bottom, sin_at] = (ci - x2).astype(BF16)
        d_ref[c] = dot(zi, w_ref[c], ((1,), (0,)))
    for n in range(XN):
        here = slice(n * 256, (n + 1) * 256)
        for k in range(0, half, LKZ):
            pair = []
            for start in (k, half + k):
                f0, f1, f2 = [d_ref[c, start : start + LKZ, here] for c in range(3)]
                last = f2 * f2
                pair.append((f0 * f0 - last, f0 * f1, f0 * f2, f1 * f1 - last, f1 * f2))
            for e in range(PRODUCTS):
                t_ref[e, k : k + LKZ, here] = (pair[0][e] + pair[1][e]).astype(BF16)
                t_ref[e, half + k : half + k + LKZ, here] = (pair[0][e] - pair[1][e]).astype(BF16)
    for e in range(PRODUCTS):
        mr = dot(zr, t_ref[e, : half + LKZ], ((1,), (0,)))
        mi = dot(zm, t_ref[e, half:], ((1,), (0,)))
        for n in range(XN):
            cos_at = slice(n * 256, n * 256 + 128)
            sin_at = slice(n * 256 + 128, (n + 1) * 256)
            for k in range(0, NZH, LKZ):
                rows = slice(k, k + LKZ)
                er, orr = mr[rows, cos_at] + mr[rows, sin_at], mr[rows, cos_at] - mr[rows, sin_at]
                ei, oi = mi[rows, cos_at] + mi[rows, sin_at], mi[rows, cos_at] - mi[rows, sin_at]
                x1, x2 = oi, -orr
                if n == 0:
                    x1 = jnp.where(first, orr, oi)
                    x2 = jnp.where(first, oi, -orr)
                top = slice(e * NZH + k, e * NZH + k + LKZ)
                bottom = slice((PRODUCTS + e) * NZH + k, (PRODUCTS + e) * NZH + k + LKZ)
                f_ref[top, cos_at] = er.astype(BF16)
                f_ref[top, sin_at] = x1.astype(BF16)
                f_ref[bottom, cos_at] = ei.astype(BF16)
                f_ref[bottom, sin_at] = x2.astype(BF16)

    masks = lane_masks(PRODUCTS * HALF)
    for m in range(NX // 256):
        res = dot(f_ref[...], x_ref[m * 256 : (m + 1) * 256, :], ((1,), (1,)))
        for side in range(2):
            for r in range(ROWS):
                four = []
                for hi in range(2):
                    for s in range(2):
                        pieces = []
                        for e in range(PRODUCTS):
                            start = (s * PRODUCTS + e) * NZH + r * LKZ + hi * HALF
                            pieces.append(
                                res[start : start + HALF, side * 128 : (side + 1) * 128]
                            )
                        four.append(jnp.concatenate(pieces, axis=0))
                parts = exchange4(*four, *masks)
                for q in range(4):
                    o_ref[r * COLS + 4 * (2 * m + side) + q] = parts[q].astype(BF16)


def middle(messages, table):
    return pl.pallas_call(
        middle_kernel,
        grid=(YPD,),
        in_specs=[
            pl.BlockSpec((DEV, MSG_IN, 128), lambda y: (0, 0, 0)),
            pl.BlockSpec((NX, MX), lambda y: (0, 0)),
            pl.BlockSpec((MZ, 2 * NZH), lambda y: (0, 0)),
            pl.BlockSpec((NZH, MZ // 2 + 16), lambda y: (0, 0)),
            pl.BlockSpec((NZH, MZ // 2), lambda y: (0, 0)),
        ],
        out_specs=pl.BlockSpec((DEV, PRODUCTS * HALF, 128), lambda y: (0, y, 0)),
        out_shape=pltpu.HBM((DEV, MSG_OUT, 128), BF16),
        scratch_shapes=[
            pltpu.VMEM((6 * NZH, NX), BF16),
            pltpu.VMEM((2 * PRODUCTS * NZH, MX), BF16),
            pltpu.VMEM((3, 2 * NZH, MX), BF16),
            pltpu.VMEM((3, MZ, MX), F32),
            pltpu.VMEM((PRODUCTS, MZ, MX), BF16),
        ],
        compiler_params=pltpu.CompilerParams(vmem_limit_bytes=26 * 2**20),
        name="middle",
    )(messages, table, *z_tables())


PACK = 2 * 6 * LKX
PARTS = 4
FIELD = (3, 2, 2, HALF, LKX, NY)


def field_block(per):
    return pl.BlockSpec((3, 2, 2, per, LKX, NY), lambda k: (0, 0, 0, k, 0, 0))


def slab_block(per):
    return pl.BlockSpec((1, 3, 2, 2, per, LKX, NY), lambda k: (0, 0, 0, 0, k, 0, 0))


def move_block(per):
    return pl.BlockSpec((SHIFT_CAP, per * PACK), lambda k: (0, k))


SLABS = 8
LINEAR_PER = 4
UPDATE_PER = 2
SETTLE_PER = 4


def wave_numbers(scal_ref, lo, hi):
    shape = (LKX, NY)
    k2 = (lax.broadcasted_iota(jnp.int32, shape, 1) - NY // 2).astype(F32)
    k1 = lax.broadcasted_iota(jnp.int32, shape, 0).astype(F32) + scal_ref[0] - SHEAR_TIME * k2
    k3 = scal_ref[1] + (lo + hi * HALF).astype(F32)
    squared = k1 * k1 + k2 * k2 + k3 * k3
    return k1, k2, k3, squared, 1.0 / jnp.maximum(squared, 1.0)


def linear_kernel(scal_ref, v_ref, reg_ref, out_ref):
    for u, hi in ((u, hi) for u in range(LINEAR_PER) for hi in range(2)):
        lo = pl.program_id(0) * LINEAR_PER + u
        k1, k2, k3, squared, inverse = wave_numbers(scal_ref, lo, hi)
        lift = 2.0 * SHEAR_RATE * k2 * inverse
        for half in range(2):
            first = v_ref[0, half, hi, u]
            lifted = lift * first
            for m, wave in enumerate((k1, k2, k3)):
                velocity = v_ref[m, half, hi, u]
                rate = wave * lifted - VISCOSITY * squared * velocity
                if m == 1:
                    rate = rate - SHEAR_RATE * first
                increment = REGISTER_WEIGHT * reg_ref[m, half, hi, u] + TIME_STEP * rate
                out_ref[0, m, half, hi, u] = velocity + UPDATE_WEIGHT * increment


def linear_part(scalars, velocity, register):
    return pl.pallas_call(
        linear_kernel,
        grid=(HALF // LINEAR_PER,),
        in_specs=[pl.BlockSpec(memory_space=pltpu.SMEM), field_block(LINEAR_PER), field_block(LINEAR_PER)],
        out_specs=slab_block(LINEAR_PER),
        out_shape=pltpu.HBM((SLABS,) + FIELD, F32),
        compiler_params=pltpu.CompilerParams(vmem_limit_bytes=60 * 2**20),
        name="linear",
    )(scalars, velocity.reshape(FIELD), register.reshape(FIELD))


def one_hot(slot_ref):
    slots = lax.broadcasted_iota(jnp.int32, (4 * SHIFT_CAP, NY), 0)
    return jnp.where(slots == slot_ref[...], 1.0, 0.0).astype(BF16)


def update_kernel(
    scal_ref, g_hbm, table_ref, lin_ref, place_ref, stay_ref, base_ref, p0, p1, p2, p3, scr_ref,
    g_ref, sems,
):
    step = pl.program_id(0)

    @pl.when(step == 0)
    def _():
        copies = []
        for part in range(PARTS):
            here = pl.ds(part * (DEV // PARTS), DEV // PARTS)
            copies.append(pltpu.make_async_copy(g_hbm.at[here], g_ref.at[here], sems.at[part]))
            copies[-1].start()

        def unpack(d, carry):
            rows = g_ref[pl.ds(d * 8, 8)].astype(F32).reshape(8 * MSG_OUT, 128)
            scr_ref[pl.ds(pl.multiple_of(d * 8 * MSG_OUT, 8), 8 * MSG_OUT), :] = rows
            return carry

        share = DEV // 8 // PARTS
        for part in range(PARTS):
            copies[part].wait()
            lax.fori_loop(part * share, (part + 1) * share, unpack, 0)

    table = table_ref[...]
    place = one_hot(place_ref)
    stay = stay_ref[...]
    weight = UPDATE_WEIGHT * TIME_STEP * FORWARD_SCALE * INVERSE_SCALE * INVERSE_SCALE
    for u in range(UPDATE_PER):
        lo = step * UPDATE_PER + u
        spectra = []
        for e in range(PRODUCTS):
            parts = [
                scr_ref[
                    pl.ds(y * PRODUCTS * HALF + e * HALF + lo, DEV, stride=MSG_OUT), :
                ].astype(BF16)
                for y in range(YPD)
            ]
            spectra.append(dot(jnp.concatenate(parts, axis=0), table, ((0,), (0,))))

        moving = []
        for hi in range(2):
            k1, k2, k3, squared, inverse = wave_numbers(scal_ref, lo, hi)
            real = []
            imag = []
            for p in spectra:
                top = p[hi * 2 * LKX : hi * 2 * LKX + LKX]
                bottom = p[hi * 2 * LKX + LKX : (hi + 1) * 2 * LKX]
                real.append(top[:, :NY] + bottom[:, NY:])
                imag.append(bottom[:, :NY] - top[:, NY:])
            for half, t, sign in ((0, imag, weight), (1, real, -weight)):
                stress = (
                    k1 * t[0] + k2 * t[1] + k3 * t[2],
                    k1 * t[1] + k2 * t[3] + k3 * t[4],
                    k1 * t[2] + k2 * t[4],
                )
                pressure = (k1 * stress[0] + k2 * stress[1] + k3 * stress[2]) * inverse
                for m, wave in enumerate((k1, k2, k3)):
                    updated = lin_ref[0, m, half, hi, u] + sign * (stress[m] - wave * pressure)
                    base_ref[m, half, hi, u] = updated * stay
                    moving.append(updated.astype(BF16))
        packed = dot(place, jnp.concatenate(moving, axis=0), ((1,), (1,))).astype(BF16)
        for position, ref in enumerate((p0, p1, p2, p3)):
            ref[:, u * PACK : (u + 1) * PACK] = packed[position * SHIFT_CAP : (position + 1) * SHIFT_CAP]


def update(scalars, gathered, linear, place, stay):
    return pl.pallas_call(
        update_kernel,
        grid=(HALF // UPDATE_PER,),
        in_specs=[
            pl.BlockSpec(memory_space=pltpu.SMEM),
            pl.BlockSpec(memory_space=pl.ANY),
            pl.BlockSpec((MY, 2 * NY), lambda lo: (0, 0)),
            slab_block(UPDATE_PER),
            pl.BlockSpec((1, NY), lambda lo: (0, 0)),
            pl.BlockSpec((1, NY), lambda lo: (0, 0)),
        ],
        out_specs=[field_block(UPDATE_PER)] + [move_block(UPDATE_PER)] * 4,
        out_shape=[jax.ShapeDtypeStruct(FIELD, F32)]
        + [jax.ShapeDtypeStruct((SHIFT_CAP, HALF * PACK), BF16)] * 4,
        scratch_shapes=[
            pltpu.VMEM((DEV * MSG_OUT, 128), F32),
            pltpu.VMEM((DEV, MSG_OUT, 128), BF16),
            pltpu.SemaphoreType.DMA((PARTS,)),
        ],
        compiler_params=pltpu.CompilerParams(vmem_limit_bytes=44 * 2**20),
        name="update",
    )(scalars, gathered, y_table(), linear, place, stay)


def settle_kernel(scal_ref, base_ref, a0, a1, a2, a3, place_ref, out_ref):
    arrived = jnp.concatenate([a0[...], a1[...], a2[...], a3[...]], axis=0)
    moved = dot(arrived, one_hot(place_ref), ((0,), (0,)))
    keep = scal_ref[2]
    for u, hi in ((u, hi) for u in range(SETTLE_PER) for hi in range(2)):
        for m in range(3):
            for half in range(2):
                start = u * PACK + (hi * 6 + half * 3 + m) * LKX
                out_ref[m, half, hi, u] = (
                    base_ref[m, half, hi, u] + moved[start : start + LKX]
                ) * keep


def settle(scalars, base, arrivals, place):
    return pl.pallas_call(
        settle_kernel,
        grid=(HALF // SETTLE_PER,),
        in_specs=[pl.BlockSpec(memory_space=pltpu.SMEM), field_block(SETTLE_PER)]
        + [move_block(SETTLE_PER)] * 4
        + [pl.BlockSpec((1, NY), lambda lo: (0, 0))],
        out_specs=field_block(SETTLE_PER),
        out_shape=jax.ShapeDtypeStruct(FIELD, F32),
        compiler_params=pltpu.CompilerParams(vmem_limit_bytes=16 * 2**20),
        name="settle",
    )(scalars, base, *arrivals, place)


def from_behind(block, axis, distance):
    return lax.ppermute(block, axis, [((i - distance) % COLS, i) for i in range(COLS)])


def local(velocity, register, offsets, remesh_flag, keep_blocks):
    row_index = lax.axis_index("row")
    col_index = lax.axis_index("col")
    moved_by = offsets * remesh_flag
    marked = jnp.stack([moved_by == value for value in OFFSET_VALUES])
    order = jnp.arange(NY, dtype=jnp.int32)
    upto = (order[:, None] <= order[None, :]).astype(BF16)
    ranked = jnp.dot(marked.astype(BF16), upto, preferred_element_type=F32).astype(jnp.int32) - 1
    slots = ranked + SHIFT_CAP * jnp.arange(4, dtype=jnp.int32)[:, None]
    sources = col_index - jnp.array(OFFSET_VALUES, dtype=jnp.int32)[:, None]
    inside = (sources >= 0) & (sources < COLS)
    place = jnp.max(jnp.where(marked, slots, -1), axis=0, keepdims=True)
    taking = jnp.max(jnp.where(marked & inside, slots, -1), axis=0, keepdims=True)
    stay = (moved_by == 0).astype(F32).reshape(1, NY)
    keep_here = jnp.sum(
        jnp.where(jnp.arange(COLS, dtype=jnp.int32) == col_index, keep_blocks, 0)
    ).astype(F32)
    scalars = jnp.stack(
        [
            (col_index * LKX - NX // 2).astype(F32),
            (row_index * LKZ).astype(F32),
            keep_here,
        ]
    )

    outgoing = y_inverse(velocity)
    table = x_table()
    messages = lax.all_to_all(outgoing, ("row", "col"), split_axis=0, concat_axis=0, tiled=True)
    returning = middle(messages, table)
    gathered = lax.all_to_all(returning, ("row", "col"), split_axis=0, concat_axis=0, tiled=True)
    linear = linear_part(scalars, velocity, register)
    base, *packed = update(scalars, gathered, linear, place, stay)
    arrivals = [
        from_behind(block, "col", value) for block, value in zip(packed, OFFSET_VALUES)
    ]
    result = settle(scalars, base, arrivals, taking)
    return result.reshape(velocity.shape)


def solution(mesh):
    placed = (P(None, None, "row", "col", None), P(None, None, "row", "col", None), P(), P(), P())
    return jax.shard_map(
        local,
        mesh=mesh,
        in_specs=placed,
        out_specs=P(None, None, "row", "col", None),
        check_vma=False,
    )
```
